128 devices in a mesh: row: 16 (over y_hi, x, core), col: 8 (over y_lo, z).
Axes of the slice: x: 4, y: 4 (y_hi: 2, y_lo: 2; y = y_hi * 2 + y_lo), z: 4, core: 2. Of those that a mesh axis runs over, the one named last changes fastest.
Arguments:
- queries: bfloat16 [1024, 32, 128], P(('row', 'col')), may hold values from -1 to 1
- documents: bfloat16 [1024, 128, 128], P(('row', 'col')), may hold values from -1 to 1
- lengths: int32 [1024], P(('row', 'col')), may hold values from 1 to 128
- positives: int32 [1024], P(('row', 'col')), may hold values from 0 to 1023
Outputs:
- query_loss: float32 [1024], P(('row', 'col'))
The draws below stay inside these ranges and needn't reach their ends.
All inputs are finite; a program needn't handle non-finite values.
Results may differ from the reference program's by a relative error of at most 0.0003.
Values may be sent and summed in bfloat16 or wider, within the bound.
No kernel may reach another device: no remote copies, remote signals or barrier semaphores. Data moves between devices by JAX's collectives and lax.ppermute only.
A program may use at most 64 MiB of HBM per device.

```python
import jax
import jax.numpy as jnp
from jax import lax

DIM = 128
QT = 32
DT = 128
NQ = 1024
ND = 1024


def draw_queries(key, part):
    own_key = jax.random.fold_in(key, 71)
    spread = 0.8 * DIM ** (-0.5)
    values = jnp.clip(spread * jax.random.normal(own_key, (NQ, QT, DIM), jnp.float32), -1.0, 1.0)
    return values.astype(jnp.bfloat16)


def draw_documents(key, part):
    own_key = jax.random.fold_in(key, 72)
    spread = 0.8 * DIM ** (-0.5)
    values = jnp.clip(spread * jax.random.normal(own_key, (ND, DT, DIM), jnp.float32), -1.0, 1.0)
    return values.astype(jnp.bfloat16)


def with_ends(array, stream_key, smallest, high):
    longest = array.shape.index(max(array.shape))
    spots = []
    for shift in (0, 1):
        where = [jax.random.randint(jax.random.fold_in(stream_key, axis), (), 0, length) for axis, length in enumerate(array.shape)]
        where[longest] = (where[longest] + shift) % array.shape[longest]
        spots.append(tuple(where))
    return array.at[spots[0]].set(smallest).at[spots[1]].set(high)


def setup_inputs(seed: int = 0) -> dict:
    key_list = jax.random.split(jax.random.key(seed), 5)
    return {
        "queries": draw_queries(jax.random.fold_in(key_list[4], 71), 0),
        "documents": draw_documents(jax.random.fold_in(key_list[4], 71), 0),
        "lengths": with_ends(jax.random.randint(key_list[2], (ND,), 1, DT + 1), jax.random.fold_in(key_list[2], 1), 1, DT).astype(jnp.int32),
        "positives": with_ends(jax.random.randint(key_list[3], (NQ,), 0, ND), jax.random.fold_in(key_list[3], 1), 0, ND - 1).astype(jnp.int32),
    }


neg_fill = -1.0e30


def reference(queries, documents, lengths, positives):
    query_flat = queries.astype(jnp.float32).reshape(NQ * QT, DIM)
    token_slots = jnp.arange(DT, dtype=jnp.int32)

    def one_document(doc_pair):
        document, doc_length = doc_pair
        similar = lax.dot_general(query_flat, document.astype(jnp.float32), (((1,), (1,)), ((), ())), precision=lax.Precision.HIGHEST, preferred_element_type=jnp.float32)
        similar = jnp.where(token_slots[None, :] < doc_length, similar, neg_fill)
        return jnp.sum(jnp.max(similar, axis=1).reshape(NQ, QT), axis=1)

    scores = lax.map(one_document, (documents, lengths)).T
    peak_score = jnp.max(scores, axis=1, keepdims=True)
    log_total = peak_score[:, 0] + jnp.log(jnp.sum(jnp.exp(scores - peak_score), axis=1))
    doc_ids = jnp.arange(ND, dtype=jnp.int32)
    positive_score = jnp.sum(jnp.where(doc_ids[None, :] == positives[:, None], scores, 0.0), axis=1)
    return log_total - positive_score
```

```python
import functools

import jax
import jax.numpy as jnp
from jax import lax
from jax.experimental import pallas as pl
from jax.experimental.pallas import tpu as pltpu
from jax.sharding import Mesh, PartitionSpec as P

neg_fill = -1e30
QUERIES, TOKENS, DOCS, SLOTS, DIM = 8, 32, 8, 128, 128
PAY = DOCS * SLOTS + 16
ROWS = 512


def index(x, y, z, core):
    return (((y // 2 * 4 + x) * 2 + core) * 2 + y % 2) * 4 + z


def everywhere():
    return [(x, y, z, c) for x in range(4) for y in range(4) for z in range(4) for c in range(2)]


def across(dim, place):
    axis = "xyz".index(dim[0])
    moved = list(place)
    moved[axis] = place[axis] ^ 1 if dim[1] == "a" else 3 - place[axis]
    return tuple(moved)


def side(dim, place):
    at = place["xyz".index(dim[0])]
    return ((0, 1, 1, 0) if dim[1] == "a" else (0, 0, 1, 1))[at]


DOC_STEPS = (("yb", "zb"), ("zb", "yb"))
QUERY_STEPS = (("xa", "xb", "ya", "za"), ("ya", "za", "xa", "xb"))


def swap(array, steps, at):
    pairs = [(index(*p), index(*across(steps[p[3]][at], p))) for p in everywhere()]
    return lax.ppermute(array, "d", pairs)


def swap_cores(array):
    pairs = [(index(x, y, z, c), index(x, y, z, 1 - c)) for x, y, z, c in everywhere()]
    return lax.ppermute(array, "d", pairs)


def member(place):
    return sum(side(dim, place) << k for k, dim in enumerate(QUERY_STEPS[place[3]]))


def owner_groups():
    groups = {}
    for p in everywhere():
        groups.setdefault((p[3], side("yb", p), side("zb", p)), []).append(p)
    return [[index(*p) for p in sorted(g, key=member)] for g in groups.values()]


def spec(space):
    return pl.BlockSpec(memory_space=space)


def pack_kernel(place_ref, lengths_ref, docs_ref, queries_ref, doc_out, query_out, wide):
    row = lax.broadcasted_iota(jnp.int32, (SLOTS, DIM), 0)
    for d in range(DOCS):
        doc = docs_ref[d].astype(jnp.float32)
        doc = jnp.where(row < lengths_ref[d], doc, doc[:1, :])
        doc_out[d * SLOTS : (d + 1) * SLOTS, :] = doc.astype(jnp.bfloat16)
    row = lax.broadcasted_iota(jnp.int32, (16, DIM), 0)
    lane = lax.broadcasted_iota(jnp.int32, (16, DIM), 1)
    facts = jnp.zeros((16, DIM), jnp.int32) + place_ref[0]
    for d in range(DOCS):
        facts = jnp.where((row == 0) & (lane == d), lengths_ref[d], facts)
    doc_out[DOCS * SLOTS :, :] = facts.astype(jnp.float32).astype(jnp.bfloat16)
    for q in range(QUERIES):
        wide[q * TOKENS : (q + 1) * TOKENS, :] = queries_ref[q].astype(jnp.float32)
    for t in range(0, TOKENS, 2):
        pair = [wide[pl.ds(t + k, QUERIES, stride=TOKENS), :] for k in range(2)]
        query_out[t * QUERIES : (t + 2) * QUERIES, :] = jnp.concatenate(pair).astype(jnp.bfloat16)


def pack(place, lengths, docs, queries):
    return pl.pallas_call(
        pack_kernel,
        out_shape=(
            jax.ShapeDtypeStruct((PAY, DIM), jnp.bfloat16),
            jax.ShapeDtypeStruct((QUERIES * TOKENS, DIM), jnp.bfloat16),
        ),
        in_specs=[spec(pltpu.SMEM), spec(pltpu.SMEM), spec(pltpu.VMEM), spec(pltpu.VMEM)],
        out_specs=(spec(pltpu.VMEM), spec(pltpu.VMEM)),
        scratch_shapes=[pltpu.VMEM((QUERIES * TOKENS, DIM), jnp.float32)],
        name="pack",
    )(place, lengths, docs, queries)


def merge(a, b, shift, axis):
    at = lax.broadcasted_iota(jnp.int32, (8, 128), axis)
    low = (at // shift) % 2 == 0
    mine = jnp.where(low, a, b)
    other = pltpu.roll(jnp.where(low, b, a), shift, axis)
    return mine + other if axis else jnp.maximum(mine, other)


def score_kernel(sizes, blocks, facts_ref, place_ref, *refs):
    doc_refs, (query_ref, out_ref, rows, best, owner, carry, scores) = refs[: len(sizes)], refs[len(sizes) :]
    doc_count = DOCS * sum(sizes)
    groups = ROWS // 16
    total = jnp.int32(0)
    first = 0
    for size, doc_ref in zip(sizes, doc_refs):
        for p in range(size):

            def copy_doc(d, at, doc_ref=doc_ref, p=p, part=first + p):
                source = pl.multiple_of(p * PAY + d * SLOTS, 16)
                rows[pl.ds(pl.multiple_of(at * 16, 16), SLOTS), :] = doc_ref[pl.ds(source, SLOTS), :]
                for k in range(SLOTS // 16):
                    owner[at + k] = part * DOCS + d
                return at + (facts_ref[part * 16 + d] + 15) // 16

            total = lax.fori_loop(0, DOCS, copy_doc, total, unroll=True)
        first += size
    for k in range(groups):
        owner[total + k] = doc_count
    carry[...] = jnp.full_like(carry, neg_fill)

    def body(i, last):
        base = i * groups
        ids = [owner[base + g] for g in range(groups)]
        drop = [jnp.where(a == b, 0.0, neg_fill) for a, b in zip(ids, [last] + ids[:-1])]
        block_rows = rows[pl.ds(pl.multiple_of(base * 16, 16), ROWS), :]
        for b in range(blocks):
            similar = lax.dot_general(
                block_rows,
                query_ref[b * 256 : (b + 1) * 256, :],
                (((1,), (1,)), ((), ())),
                preferred_element_type=jnp.float32,
            )
            for h in range(2):
                run = carry[2 * b + h]
                for g in range(groups):
                    tile = similar[16 * g : 16 * g + 16, 128 * h : 128 * h + 128]
                    run = jnp.maximum(jnp.maximum(tile[:8], tile[8:]), run + drop[g])
                    best[2 * b + h, pl.ds(pl.multiple_of(ids[g] * 8, 8), 8), :] = run
                carry[2 * b + h] = run
        return ids[-1]

    lax.fori_loop(0, (total + groups - 1) // groups, body, jnp.int32(-1))

    def reduce(part, carried):
        columns = []
        for b in range(blocks):
            halves = []
            for h in range(2):
                v = [best[2 * b + h, pl.ds(pl.multiple_of(part * 64 + d * 8, 8), 8), :] for d in range(8)]
                for shift in (1, 2, 4):
                    v = [merge(v[2 * k], v[2 * k + 1], shift, 0) for k in range(len(v) // 2)]
                halves.append(v[0])
            columns.append(halves[0] + halves[1])
        for shift in (8, 16, 32, 64):
            columns = [merge(columns[2 * k], columns[2 * k + 1], shift, 1) for k in range(len(columns) // 2)]
        scores[pl.ds(pl.multiple_of(part * 8, 8), 8), :] = columns[0]
        ids = facts_ref[part * 16 + 8] * DOCS + lax.broadcasted_iota(jnp.int32, (8, 128), 0)
        scores[pl.ds(pl.multiple_of(doc_count + part * 8, 8), 8), :] = ids.astype(jnp.float32)
        return carried

    lax.fori_loop(0, doc_count // 8, reduce, 0, unroll=True)
    turned = scores[...].T
    for b in range(blocks):
        out_ref[b ^ place_ref[1]] = turned[b * 8 : (b + 1) * 8, :]


def score(facts, place, docs, queries):
    sizes = [d.shape[0] // PAY for d in docs]
    doc_count = DOCS * sum(sizes)
    blocks = queries.shape[0] // 256
    return pl.pallas_call(
        functools.partial(score_kernel, sizes, blocks),
        out_shape=jax.ShapeDtypeStruct((blocks, 8, 128), jnp.float32),
        in_specs=[spec(pltpu.SMEM), spec(pltpu.SMEM)] + [spec(pltpu.VMEM)] * (len(docs) + 1),
        out_specs=spec(pltpu.VMEM),
        scratch_shapes=[
            pltpu.VMEM((doc_count * SLOTS + ROWS, DIM), jnp.bfloat16),
            pltpu.VMEM((blocks * 2, (doc_count + 1) * 8, 128), jnp.float32),
            pltpu.SMEM((doc_count * 8 + ROWS // 16,), jnp.int32),
            pltpu.VMEM((blocks * 2, 8, 128), jnp.float32),
            pltpu.VMEM((2 * doc_count, 128), jnp.float32),
        ],
        compiler_params=pltpu.CompilerParams(vmem_limit_bytes=40 * 2**20),
        name="score",
    )(facts, place, *docs, queries)


def finish_kernel(positives_ref, given_ref, out_ref):
    lane = lax.broadcasted_iota(jnp.int32, (8, 128), 1)
    row = lax.broadcasted_iota(jnp.int32, (8, 128), 0)
    wanted = jnp.zeros((8, 128), jnp.int32)
    for q in range(QUERIES):
        wanted = jnp.where(row == q, positives_ref[q], wanted)
    wanted = wanted.astype(jnp.float32)
    count = given_ref.shape[0]
    given = [given_ref[k] for k in range(count)]
    real = [jnp.where(lane < 64, g, neg_fill) for g in given]
    peak = jnp.max(functools.reduce(jnp.maximum, real), axis=1, keepdims=True)
    total = jnp.sum(sum(jnp.where(lane < 64, jnp.exp(r - peak), 0.0) for r in real), axis=1, keepdims=True)
    chosen = [jnp.where((lane < 64) & (pltpu.roll(g, 64, 1) == wanted), g, 0.0) for g in given]
    loss = peak + jnp.log(total) - jnp.sum(sum(chosen), axis=1, keepdims=True)
    out_ref[...] = jnp.sum(jnp.where(row == lane, loss, 0.0), axis=0, keepdims=True)


def finish(positives, given):
    return pl.pallas_call(
        finish_kernel,
        out_shape=jax.ShapeDtypeStruct((1, 128), jnp.float32),
        in_specs=[spec(pltpu.SMEM), spec(pltpu.VMEM)],
        out_specs=spec(pltpu.VMEM),
        name="finish",
    )(positives, given)


def local(queries, documents, lengths, positives):
    here = lax.axis_index("d")
    members = [0] * 128
    for p in everywhere():
        members[index(*p)] = member(p)
    place = jnp.stack([here, jnp.asarray(members, jnp.int32)[here]])
    own, query = pack(place, lengths, documents, queries)
    for at in range(4):
        query = jnp.concatenate([query, swap(query, QUERY_STEPS, at)])
        if at == 0:
            near = swap(own, DOC_STEPS, 0)
        if at == 1:
            far = swap(jnp.concatenate([own, near]), DOC_STEPS, 1)
    docs = [own, near, far] + [swap_cores(d) for d in (own, near, far)]
    facts = jnp.stack(
        [d[k * PAY + DOCS * SLOTS : k * PAY + DOCS * SLOTS + 2, :8] for d in docs for k in range(d.shape[0] // PAY)]
    )
    facts = facts.astype(jnp.int32).reshape(-1)
    given = score(facts, place, docs, query)
    given = lax.all_to_all(given, "d", 0, 0, tiled=True, axis_index_groups=owner_groups())
    return finish(positives, given)[0, :QUERIES]


def solution(mesh):
    flat = Mesh(mesh.devices.reshape(-1), ("d",))
    placed = P("d")
    return jax.shard_map(local, mesh=flat, in_specs=(placed,) * 4, out_specs=placed, check_vma=False)
```

```python
import functools

import jax
import jax.numpy as jnp
from jax import lax
from jax.experimental import pallas as pl
from jax.experimental.pallas import tpu as pltpu
from jax.sharding import Mesh, PartitionSpec as P

neg_fill = -1e30
QUERIES, TOKENS, DOCS, SLOTS, DIM = 8, 32, 8, 128, 128
PAY = DOCS * SLOTS + 16
LARGE, SMALL = 64, 16


def index(x, y, z, core):
    return (((y // 2 * 4 + x) * 2 + core) * 2 + y % 2) * 4 + z


def everywhere():
    return [(x, y, z, c) for x in range(4) for y in range(4) for z in range(4) for c in range(2)]


def across(dim, place):
    axis = "xyz".index(dim[0])
    moved = list(place)
    moved[axis] = place[axis] ^ 1 if dim[1] == "a" else 3 - place[axis]
    return tuple(moved)


def side(dim, place):
    at = place["xyz".index(dim[0])]
    return ((0, 1, 1, 0) if dim[1] == "a" else (0, 0, 1, 1))[at]


DOC_STEPS = (("yb", "zb"), ("zb", "yb"))
QUERY_STEPS = (("xb", "xa", "ya", "za"), ("xb", "ya", "za", "xa"))


def swap(array, steps, at):
    pairs = [(index(*p), index(*across(steps[p[3]][at], p))) for p in everywhere()]
    return lax.ppermute(array, "d", pairs)


def swap_cores(array):
    pairs = [(index(x, y, z, c), index(x, y, z, 1 - c)) for x, y, z, c in everywhere()]
    return lax.ppermute(array, "d", pairs)


def member(place):
    return sum(side(dim, place) << k for k, dim in enumerate(QUERY_STEPS[place[3]]))


def owner_groups():
    groups = {}
    for p in everywhere():
        groups.setdefault((p[3], side("yb", p), side("zb", p)), []).append(p)
    return [[index(*p) for p in sorted(g, key=member)] for g in groups.values()]


def spec(space):
    return pl.BlockSpec(memory_space=space)


def pack_docs_kernel(lengths_ref, docs_ref, out_ref):
    row = lax.broadcasted_iota(jnp.int32, (SLOTS, DIM), 0)
    for d in range(DOCS):
        doc = docs_ref[d].astype(jnp.float32)
        doc = jnp.where(row < lengths_ref[d], doc, doc[:1, :])
        out_ref[d * SLOTS : (d + 1) * SLOTS, :] = doc.astype(jnp.bfloat16)
    lane = lax.broadcasted_iota(jnp.int32, (16, DIM), 1)
    facts = jnp.zeros((16, DIM), jnp.int32)
    for d in range(DOCS):
        facts = jnp.where(lane == d, lengths_ref[d], facts)
    out_ref[DOCS * SLOTS :, :] = facts.astype(jnp.float32).astype(jnp.bfloat16)


def pack_docs(lengths, docs):
    return pl.pallas_call(
        pack_docs_kernel,
        out_shape=jax.ShapeDtypeStruct((PAY, DIM), jnp.bfloat16),
        in_specs=[spec(pltpu.SMEM), spec(pltpu.VMEM)],
        out_specs=spec(pltpu.VMEM),
        cost_estimate=pl.CostEstimate(flops=10**6, bytes_accessed=10**6, transcendentals=0),
        name="pack_docs",
    )(lengths, docs)


def pack_queries_kernel(queries_ref, out_ref, wide):
    for q in range(QUERIES):
        wide[q * TOKENS : (q + 1) * TOKENS, :] = queries_ref[q].astype(jnp.float32)
    for t in range(0, TOKENS, 2):
        pair = [wide[pl.ds(t + k, QUERIES, stride=TOKENS), :] for k in range(2)]
        out_ref[t * QUERIES : (t + 2) * QUERIES, :] = jnp.concatenate(pair).astype(jnp.bfloat16)


def pack_queries(queries):
    return pl.pallas_call(
        pack_queries_kernel,
        out_shape=jax.ShapeDtypeStruct((QUERIES * TOKENS, DIM), jnp.bfloat16),
        in_specs=[spec(pltpu.VMEM)],
        out_specs=spec(pltpu.VMEM),
        scratch_shapes=[pltpu.VMEM((QUERIES * TOKENS, DIM), jnp.float32)],
        name="pack_queries",
    )(queries)


def merge(a, b, shift, axis):
    at = lax.broadcasted_iota(jnp.int32, (8, 128), axis)
    low = (at // shift) % 2 == 0
    mine = jnp.where(low, a, b)
    other = pltpu.roll(jnp.where(low, b, a), shift, axis)
    return mine + other if axis else jnp.maximum(mine, other)


def doc_sources(me):
    core = (me >> 3) & 1
    y_pair, z_pair = 68, 3
    one = jnp.where(core == 0, y_pair, z_pair)
    two = jnp.where(core == 0, z_pair, y_pair)
    both = y_pair ^ z_pair
    masks = [0, one, two, both, 8, 8 ^ two, 8 ^ one, 8 ^ both]
    return [me ^ m for m in masks]


def my_member(me):
    yh, x1, x0, core, yl, z1, z0 = [(me >> k) & 1 for k in (6, 5, 4, 3, 2, 1, 0)]
    bits = {"xb": x1, "xa": x0 ^ x1, "ya": yl ^ yh, "za": z0 ^ z1}
    places = [sum(bits[dim] << k for k, dim in enumerate(steps)) for steps in QUERY_STEPS]
    return jnp.where(core == 0, places[0], places[1])


def score_kernel(sizes, blocks, first_block, aliased, facts_ref, *refs):
    doc_refs, rest = refs[: len(sizes)], refs[len(sizes) + aliased :]
    query_ref, out_ref, rows, best, owner, carry, scores = rest
    me = lax.axis_index("d")
    doc_count = DOCS * sum(sizes)
    total = jnp.int32(0)
    first = 0
    for size, doc_ref in zip(sizes, doc_refs):
        for p in range(size):
            part = first + p
            for d in range(DOCS):
                source = p * PAY + d * SLOTS
                rows[pl.ds(pl.multiple_of(total * 16, 16), SLOTS), :] = doc_ref[source : source + SLOTS, :]
                for k in range(SLOTS // 16):
                    owner[total + k] = part * DOCS + d
                total = total + (facts_ref[part * 8 + d] + 15) // 16
        first += size
    for k in range(SMALL):
        owner[total + k] = doc_count
    carry[...] = jnp.full_like(carry, neg_fill)

    def step(groups, base, last):
        ids = [owner[base + g] for g in range(groups)]
        drop = [jnp.where(a == b, 0.0, neg_fill) for a, b in zip(ids, [last] + ids[:-1])]
        block_rows = rows[pl.ds(pl.multiple_of(base * 16, 16), groups * 16), :]
        for b in range(blocks):
            similar = lax.dot_general(
                block_rows,
                query_ref[b * 256 : (b + 1) * 256, :],
                (((1,), (1,)), ((), ())),
                preferred_element_type=jnp.float32,
            )
            for h in range(2):
                run = carry[2 * b + h]
                for g in range(groups):
                    tile = similar[16 * g : 16 * g + 16, 128 * h : 128 * h + 128]
                    run = jnp.maximum(jnp.maximum(tile[:8], tile[8:]), run + drop[g])
                    best[2 * b + h, pl.ds(pl.multiple_of(ids[g] * 8, 8), 8), :] = run
                carry[2 * b + h] = run
        return ids[-1]

    large = total // LARGE
    last = lax.fori_loop(0, large, lambda i, last: step(LARGE, i * LARGE, last), jnp.int32(-1))
    small = (total - large * LARGE + SMALL - 1) // SMALL
    lax.fori_loop(0, small, lambda i, last: step(SMALL, large * LARGE + i * SMALL, last), last)

    for part, source in enumerate(doc_sources(me)):
        columns = []
        for b in range(blocks):
            halves = []
            for h in range(2):
                v = [best[2 * b + h, (part * 8 + d) * 8 : (part * 8 + d + 1) * 8, :] for d in range(8)]
                for shift in (1, 2, 4):
                    v = [merge(v[2 * k], v[2 * k + 1], shift, 0) for k in range(len(v) // 2)]
                halves.append(v[0])
            columns.append(halves[0] + halves[1])
        for shift in (8, 16, 32, 64):
            if len(columns) > 1:
                columns = [merge(columns[2 * k], columns[2 * k + 1], shift, 1) for k in range(len(columns) // 2)]
            else:
                columns = [columns[0] + pltpu.roll(columns[0], shift, 1)]
        scores[part * 8 : part * 8 + 8, :] = columns[0]
        ids = source * DOCS + lax.broadcasted_iota(jnp.int32, (8, 128), 0)
        scores[doc_count + part * 8 : doc_count + part * 8 + 8, :] = ids.astype(jnp.float32)
    turned = scores[...].T
    at = my_member(me)
    for b in range(blocks):
        out_ref[(b + first_block) ^ at] = turned[b * 8 : (b + 1) * 8, :]


def score(facts, docs, queries, first_block, so_far=None):
    sizes = [d.shape[0] // PAY for d in docs]
    doc_count = DOCS * sum(sizes)
    blocks = queries.shape[0] // 256
    extra = [] if so_far is None else [so_far]
    return pl.pallas_call(
        functools.partial(score_kernel, sizes, blocks, first_block, len(extra)),
        out_shape=jax.ShapeDtypeStruct((16, 8, 128), jnp.float32),
        in_specs=[spec(pltpu.SMEM)]
        + [spec(pltpu.VMEM)] * len(docs)
        + [spec(pltpu.VMEM)] * len(extra)
        + [spec(pltpu.VMEM)],
        out_specs=spec(pltpu.VMEM),
        input_output_aliases={1 + len(docs): 0} if extra else {},
        scratch_shapes=[
            pltpu.VMEM((doc_count * SLOTS + SMALL * 16, DIM), jnp.bfloat16),
            pltpu.VMEM((blocks * 2, (doc_count + 1) * 8, 128), jnp.float32),
            pltpu.SMEM((doc_count * 8 + SMALL,), jnp.int32),
            pltpu.VMEM((blocks * 2, 8, 128), jnp.float32),
            pltpu.VMEM((2 * doc_count, 128), jnp.float32),
        ],
        compiler_params=pltpu.CompilerParams(vmem_limit_bytes=24 * 2**20),
        cost_estimate=pl.CostEstimate(flops=6 * 10**9, bytes_accessed=10**6, transcendentals=0),
        name="score",
    )(facts, *docs, *extra, queries)


def finish_kernel(positives_ref, given_ref, out_ref):
    lane = lax.broadcasted_iota(jnp.int32, (8, 128), 1)
    row = lax.broadcasted_iota(jnp.int32, (8, 128), 0)
    wanted = jnp.zeros((8, 128), jnp.int32)
    for q in range(QUERIES):
        wanted = jnp.where(row == q, positives_ref[q], wanted)
    wanted = wanted.astype(jnp.float32)
    count = given_ref.shape[0]
    given = [given_ref[k] for k in range(count)]
    real = [jnp.where(lane < 64, g, neg_fill) for g in given]
    peak = jnp.max(functools.reduce(jnp.maximum, real), axis=1, keepdims=True)
    total = jnp.sum(sum(jnp.where(lane < 64, jnp.exp(r - peak), 0.0) for r in real), axis=1, keepdims=True)
    chosen = [jnp.where((lane < 64) & (pltpu.roll(g, 64, 1) == wanted), g, 0.0) for g in given]
    loss = peak + jnp.log(total) - jnp.sum(sum(chosen), axis=1, keepdims=True)
    out_ref[...] = jnp.sum(jnp.where(row == lane, loss, 0.0), axis=0)[:QUERIES]


def finish(positives, given):
    return pl.pallas_call(
        finish_kernel,
        out_shape=jax.ShapeDtypeStruct((QUERIES,), jnp.float32),
        in_specs=[spec(pltpu.SMEM), spec(pltpu.VMEM)],
        out_specs=spec(pltpu.VMEM),
        name="finish",
    )(positives, given)


def local(queries, documents, lengths, positives):
    query = [pack_queries(queries)]
    own = pack_docs(lengths, documents)
    for at in range(4):
        held = query[0] if at == 0 else jnp.concatenate(query)
        query = [held, swap(held, QUERY_STEPS, at)]
        if at == 0:
            near = swap(own, DOC_STEPS, 0)
        if at == 1:
            far = swap(jnp.concatenate([own, near]), DOC_STEPS, 1)
    docs = [own, near, far] + [swap_cores(d) for d in (own, near, far)]
    facts = jnp.stack([d[(k + 1) * PAY - 16, :8] for d in docs for k in range(d.shape[0] // PAY)])
    facts = facts.astype(jnp.int32).reshape(-1)
    given = score(facts, docs, query[0], 0)
    given = score(facts, docs, query[1], 8, given)
    given = lax.all_to_all(given, "d", 0, 0, tiled=True, axis_index_groups=owner_groups())
    return finish(positives, given)


def solution(mesh):
    flat = Mesh(mesh.devices.reshape(-1), ("d",))
    placed = P("d")
    return jax.shard_map(local, mesh=flat, in_specs=(placed,) * 4, out_specs=placed, check_vma=False)
```

```python
import functools

import jax
import jax.numpy as jnp
from jax import lax
from jax.experimental import pallas as pl
from jax.experimental.pallas import tpu as pltpu
from jax.sharding import Mesh, PartitionSpec as P

neg_fill = -1e30
QUERIES, TOKENS, DOCS, SLOTS, DIM = 8, 32, 8, 128, 128
PAY = DOCS * SLOTS + 16
LARGE, SMALL = 64, 16


def index(x, y, z, core):
    return (((y // 2 * 4 + x) * 2 + core) * 2 + y % 2) * 4 + z


def everywhere():
    return [(x, y, z, c) for x in range(4) for y in range(4) for z in range(4) for c in range(2)]


def across(dim, place):
    axis = "xyz".index(dim[0])
    moved = list(place)
    moved[axis] = place[axis] ^ 1 if dim[1] == "a" else 3 - place[axis]
    return tuple(moved)


def side(dim, place):
    at = place["xyz".index(dim[0])]
    return ((0, 1, 1, 0) if dim[1] == "a" else (0, 0, 1, 1))[at]


DOC_STEPS = (("yb", "zb"), ("zb", "yb"))
QUERY_STEPS = (("xb", "xa", "ya", "za"), ("xb", "ya", "za", "xa"))


def swap(array, steps, at):
    pairs = [(index(*p), index(*across(steps[p[3]][at], p))) for p in everywhere()]
    return lax.ppermute(array, "d", pairs)


def swap_cores(array):
    pairs = [(index(x, y, z, c), index(x, y, z, 1 - c)) for x, y, z, c in everywhere()]
    return lax.ppermute(array, "d", pairs)


def member(place):
    return sum(side(dim, place) << k for k, dim in enumerate(QUERY_STEPS[place[3]]))


def owner_groups():
    groups = {}
    for p in everywhere():
        groups.setdefault((p[3], side("yb", p), side("zb", p)), []).append(p)
    return [[index(*p) for p in sorted(g, key=member)] for g in groups.values()]


def spec(space):
    return pl.BlockSpec(memory_space=space)


def pack_docs_kernel(lengths_ref, docs_ref, out_ref):
    row = lax.broadcasted_iota(jnp.int32, (SLOTS, DIM), 0)
    for d in range(DOCS):
        doc = docs_ref[d].astype(jnp.float32)
        doc = jnp.where(row < lengths_ref[d], doc, doc[:1, :])
        out_ref[d * SLOTS : (d + 1) * SLOTS, :] = doc.astype(jnp.bfloat16)
    lane = lax.broadcasted_iota(jnp.int32, (16, DIM), 1)
    facts = jnp.zeros((16, DIM), jnp.int32)
    for d in range(DOCS):
        facts = jnp.where(lane == d, lengths_ref[d], facts)
    out_ref[DOCS * SLOTS :, :] = facts.astype(jnp.float32).astype(jnp.bfloat16)


def pack_docs(lengths, docs):
    return pl.pallas_call(
        pack_docs_kernel,
        out_shape=jax.ShapeDtypeStruct((PAY, DIM), jnp.bfloat16),
        in_specs=[spec(pltpu.SMEM), spec(pltpu.VMEM)],
        out_specs=spec(pltpu.VMEM),
        cost_estimate=pl.CostEstimate(flops=10**6, bytes_accessed=10**6, transcendentals=0),
        name="pack_docs",
    )(lengths, docs)


def lower_half(shift, axis):
    return (lax.broadcasted_iota(jnp.int32, (8, 128), axis) // shift) % 2 == 0


def merge_max(a, b, shift):
    low = lower_half(shift, 0)
    return jnp.maximum(jnp.where(low, a, b), pltpu.roll(jnp.where(low, b, a), shift, 0))


def merge_sum(a, b, shift):
    return jnp.where(lower_half(shift, 1), a + pltpu.roll(a, 128 - shift, 1), b + pltpu.roll(b, shift, 1))


def doc_sources(me):
    core = (me >> 3) & 1
    y_pair, z_pair = 68, 3
    one = jnp.where(core == 0, y_pair, z_pair)
    two = jnp.where(core == 0, z_pair, y_pair)
    both = y_pair ^ z_pair
    masks = [0, one, two, both, 8, 8 ^ two, 8 ^ one, 8 ^ both]
    return [me ^ m for m in masks]


def my_member(me):
    yh, x1, x0, core, yl, z1, z0 = [(me >> k) & 1 for k in (6, 5, 4, 3, 2, 1, 0)]
    bits = {"xb": x1, "xa": x0 ^ x1, "ya": yl ^ yh, "za": z0 ^ z1}
    places = [sum(bits[dim] << k for k, dim in enumerate(steps)) for steps in QUERY_STEPS]
    return jnp.where(core == 0, places[0], places[1])


def score_kernel(sizes, blocks, first_block, aliased, facts_ref, *refs):
    doc_refs, rest = refs[: len(sizes)], refs[len(sizes) + aliased :]
    query_ref, out_ref, rows, best, owner, carry, scores, turned = rest
    me = lax.axis_index("d")
    doc_count = DOCS * sum(sizes)
    total = jnp.int32(0)
    first = 0
    for size, doc_ref in zip(sizes, doc_refs):
        for p in range(size):
            part = first + p
            for d in range(DOCS):
                source = p * PAY + d * SLOTS
                rows[pl.ds(pl.multiple_of(total * 16, 16), SLOTS), :] = doc_ref[source : source + SLOTS, :]
                for k in range(SLOTS // 16):
                    owner[total + k] = part * DOCS + d
                total = total + ((facts_ref[part * 8 + d] + 15) >> 4)
        first += size
    for k in range(SMALL):
        owner[total + k] = doc_count
    carry[...] = jnp.full_like(carry, neg_fill)

    def step(groups, base, last):
        ids = [owner[base + g] for g in range(groups)]
        drop = [jnp.where(a == b, 0.0, neg_fill) for a, b in zip(ids, [last] + ids[:-1])]
        block_rows = rows[pl.ds(pl.multiple_of(base * 16, 16), groups * 16), :]
        for b in range(blocks):
            similar = lax.dot_general(
                block_rows,
                query_ref[b * 256 : (b + 1) * 256, :],
                (((1,), (1,)), ((), ())),
                preferred_element_type=jnp.float32,
            )
            for h in range(2):
                run = carry[2 * b + h]
                for g in range(groups):
                    tile = similar[16 * g : 16 * g + 16, 128 * h : 128 * h + 128]
                    run = jnp.maximum(jnp.maximum(tile[:8], tile[8:]), run + drop[g])
                    best[2 * b + h, pl.ds(pl.multiple_of(ids[g] * 8, 8), 8), :] = run
                carry[2 * b + h] = run
        return ids[-1]

    large = total >> 6
    last = lax.fori_loop(0, large, lambda i, last: step(LARGE, i * LARGE, last), jnp.int32(-1))
    small = (total - large * LARGE + SMALL - 1) >> 4
    lax.fori_loop(0, small, lambda i, last: step(SMALL, large * LARGE + i * SMALL, last), last)

    for part, source in enumerate(doc_sources(me)):
        columns = []
        for half in range(2 * blocks):
            v = [best[half, (part * 8 + d) * 8 : (part * 8 + d + 1) * 8, :] for d in range(8)]
            for shift in (1, 2, 4):
                v = [merge_max(v[2 * k], v[2 * k + 1], shift) for k in range(len(v) // 2)]
            columns.append(v[0])
        for shift in (1, 2, 4, 8, 16):
            columns = [merge_sum(a, b, shift) for a, b in zip(columns[::2], columns[-1:] if len(columns) == 1 else columns[1::2])]
        scores[part * 8 : part * 8 + 8, :] = columns[0]
        ids = source * DOCS + lax.broadcasted_iota(jnp.int32, (8, 128), 0)
        scores[doc_count + part * 8 : doc_count + part * 8 + 8, :] = ids.astype(jnp.float32)
    turned[...] = scores[...].T
    at = my_member(me)
    for b in range(blocks):
        quarters = [turned[pl.ds(2 * b + h, 4, stride=32), :] for h in range(2)]
        out_ref[(b + first_block) ^ at] = jnp.concatenate(quarters)


def score(facts, docs, queries, first_block, so_far=None):
    sizes = [d.shape[0] // PAY for d in docs]
    doc_count = DOCS * sum(sizes)
    blocks = queries.shape[0] // 256
    extra = [] if so_far is None else [so_far]
    return pl.pallas_call(
        functools.partial(score_kernel, sizes, blocks, first_block, len(extra)),
        out_shape=jax.ShapeDtypeStruct((16, 8, 128), jnp.float32),
        in_specs=[spec(pltpu.SMEM)]
        + [spec(pltpu.VMEM)] * len(docs)
        + [spec(pltpu.VMEM)] * len(extra)
        + [spec(pltpu.VMEM)],
        out_specs=spec(pltpu.VMEM),
        input_output_aliases={1 + len(docs): 0} if extra else {},
        scratch_shapes=[
            pltpu.VMEM((doc_count * SLOTS + SMALL * 16, DIM), jnp.bfloat16),
            pltpu.VMEM((blocks * 2, (doc_count + 1) * 8, 128), jnp.float32),
            pltpu.SMEM((doc_count * 8 + SMALL,), jnp.int32),
            pltpu.VMEM((blocks * 2, 8, 128), jnp.float32),
            pltpu.VMEM((2 * doc_count, 128), jnp.float32),
            pltpu.VMEM((128, 128), jnp.float32),
        ],
        compiler_params=pltpu.CompilerParams(vmem_limit_bytes=24 * 2**20),
        cost_estimate=pl.CostEstimate(flops=6 * 10**9, bytes_accessed=10**6, transcendentals=0),
        name="score",
    )(facts, *docs, *extra, queries)


def finish_kernel(positives_ref, given_ref, out_ref):
    lane = lax.broadcasted_iota(jnp.int32, (8, 128), 1)
    row = lax.broadcasted_iota(jnp.int32, (8, 128), 0)
    wanted = jnp.zeros((8, 128), jnp.int32)
    for q in range(QUERIES):
        wanted = jnp.where(row == q, positives_ref[q], wanted)
    wanted = wanted.astype(jnp.float32)
    count = given_ref.shape[0]
    given = [given_ref[k] for k in range(count)]
    real = [jnp.where(lane < 64, g, neg_fill) for g in given]
    peak = jnp.max(functools.reduce(jnp.maximum, real), axis=1, keepdims=True)
    total = jnp.sum(sum(jnp.where(lane < 64, jnp.exp(r - peak), 0.0) for r in real), axis=1, keepdims=True)
    chosen = [jnp.where((lane < 64) & (pltpu.roll(g, 64, 1) == wanted), g, 0.0) for g in given]
    loss = peak + jnp.log(total) - jnp.sum(sum(chosen), axis=1, keepdims=True)
    out_ref[...] = jnp.sum(jnp.where(row == lane, loss, 0.0), axis=0)[:QUERIES]


def finish(positives, given):
    return pl.pallas_call(
        finish_kernel,
        out_shape=jax.ShapeDtypeStruct((QUERIES,), jnp.float32),
        in_specs=[spec(pltpu.SMEM), spec(pltpu.VMEM)],
        out_specs=spec(pltpu.VMEM),
        name="finish",
    )(positives, given)


def local(queries, documents, lengths, positives):
    query = [queries.reshape(QUERIES * TOKENS, DIM)]
    own = pack_docs(lengths, documents)
    for at in range(4):
        held = query[0] if at == 0 else jnp.concatenate(query)
        query = [held, swap(held, QUERY_STEPS, at)]
        if at == 0:
            near = swap(own, DOC_STEPS, 0)
        if at == 1:
            far = swap(jnp.concatenate([own, near]), DOC_STEPS, 1)
    docs = [own, near, far] + [swap_cores(d) for d in (own, near, far)]
    facts = jnp.stack([d[(k + 1) * PAY - 16, :8] for d in docs for k in range(d.shape[0] // PAY)])
    facts = facts.astype(jnp.int32).reshape(-1)
    given = score(facts, docs, query[0], 0)
    given = score(facts, docs, query[1], 8, given)
    given = lax.all_to_all(given, "d", 0, 0, tiled=True, axis_index_groups=owner_groups())
    return finish(positives, given)


def solution(mesh):
    flat = Mesh(mesh.devices.reshape(-1), ("d",))
    placed = P("d")
    return jax.shard_map(local, mesh=flat, in_specs=(placed,) * 4, out_specs=placed, check_vma=False)
```

```python
import functools

import jax
import jax.numpy as jnp
from jax import lax
from jax.experimental import pallas as pl
from jax.experimental.pallas import tpu as pltpu
from jax.sharding import Mesh, PartitionSpec as P

neg_fill = -1e30
QUERIES, TOKENS, DOCS, SLOTS, DIM = 8, 32, 8, 128, 128
PAY = DOCS * SLOTS + 16
LARGE, SMALL = 64, 16


def index(x, y, z, core):
    return (((y // 2 * 4 + x) * 2 + core) * 2 + y % 2) * 4 + z


def everywhere():
    return [(x, y, z, c) for x in range(4) for y in range(4) for z in range(4) for c in range(2)]


def across(dim, place):
    axis = "xyz".index(dim[0])
    moved = list(place)
    moved[axis] = place[axis] ^ 1 if dim[1] == "a" else 3 - place[axis]
    return tuple(moved)


def side(dim, place):
    at = place["xyz".index(dim[0])]
    return ((0, 1, 1, 0) if dim[1] == "a" else (0, 0, 1, 1))[at]


DOC_STEPS = (("xb", "yb", "zb"), ("yb", "zb", "xb"))
QUERY_STEPS = (("xa", "ya", "za"), ("ya", "za", "xa"))


def swap(array, steps, at):
    pairs = [(index(*p), index(*across(steps[p[3]][at], p))) for p in everywhere()]
    return lax.ppermute(array, "d", pairs)


def swap_cores(array):
    pairs = [(index(x, y, z, c), index(x, y, z, 1 - c)) for x, y, z, c in everywhere()]
    return lax.ppermute(array, "d", pairs)


def member(place):
    return sum(side(dim, place) << k for k, dim in enumerate(QUERY_STEPS[place[3]]))


def member(place):
    return place[3] * 8 + sum(side(dim, place) << k for k, dim in enumerate(QUERY_STEPS[0]))


def owner_groups():
    groups = {}
    for p in everywhere():
        groups.setdefault(tuple(side(dim, p) for dim in DOC_STEPS[0]), []).append(p)
    return [[index(*p) for p in sorted(g, key=member)] for g in groups.values()]


def spec(space):
    return pl.BlockSpec(memory_space=space)


def pack_docs_kernel(lengths_ref, docs_ref, out_ref):
    row = lax.broadcasted_iota(jnp.int32, (SLOTS, DIM), 0)
    for d in range(DOCS):
        doc = docs_ref[d].astype(jnp.float32)
        doc = jnp.where(row < lengths_ref[d], doc, doc[:1, :])
        out_ref[d * SLOTS : (d + 1) * SLOTS, :] = doc.astype(jnp.bfloat16)
    lane = lax.broadcasted_iota(jnp.int32, (16, DIM), 1)
    facts = jnp.zeros((16, DIM), jnp.int32)
    for d in range(DOCS):
        facts = jnp.where(lane == d, lengths_ref[d], facts)
    out_ref[DOCS * SLOTS :, :] = facts.astype(jnp.float32).astype(jnp.bfloat16)


def pack_docs(lengths, docs):
    return pl.pallas_call(
        pack_docs_kernel,
        out_shape=pltpu.VMEM((PAY, DIM), jnp.bfloat16),
        in_specs=[spec(pltpu.SMEM), spec(pltpu.VMEM)],
        out_specs=spec(pltpu.VMEM),
        cost_estimate=pl.CostEstimate(flops=10**6, bytes_accessed=10**6, transcendentals=0),
        name="pack_docs",
    )(lengths, docs)


def lower_half(shift, axis):
    return (lax.broadcasted_iota(jnp.int32, (8, 128), axis) // shift) % 2 == 0


def merge_max(a, b, shift):
    low = lower_half(shift, 0)
    return jnp.maximum(jnp.where(low, a, b), pltpu.roll(jnp.where(low, b, a), shift, 0))


def merge_sum(a, b, shift):
    return jnp.where(lower_half(shift, 1), a + pltpu.roll(a, 128 - shift, 1), b + pltpu.roll(b, shift, 1))


def doc_sources(me):
    flips = {"xb": 48, "yb": 68, "zb": 3}
    first, second, third = (
        jnp.where((me >> 3) & 1 == 0, flips[a], flips[b]) for a, b in zip(DOC_STEPS[0], DOC_STEPS[1])
    )
    masks = [0, first, second, first ^ second]
    return [me ^ m for m in masks] + [me ^ third ^ m for m in masks]


def block_member(me, block):
    yh, x1, x0, core, yl, z1, z0 = [(me >> k) & 1 for k in (6, 5, 4, 3, 2, 1, 0)]
    mine = (x0 ^ x1) | (yl ^ yh) << 1 | (z0 ^ z1) << 2
    flips = []
    for steps in QUERY_STEPS:
        flips.append(sum(((block >> k) & 1) << QUERY_STEPS[0].index(dim) for k, dim in enumerate(steps)))
    other = block >> 3
    return ((core ^ other) << 3) | (mine ^ jnp.where(core == other, flips[0], flips[1]))


def score_kernel(sizes, blocks, final, facts_ref, *refs):
    doc_refs, rest = refs[: len(sizes)], refs[len(sizes) :]
    query_ref, rest = rest[0], rest[1:]
    if final:
        earlier_ref, rest = rest[0], rest[1:]
    out_ref, rows, best, owner, carry = rest[:5]
    doc_count = DOCS * sum(sizes)
    total = jnp.int32(0)
    first = 0
    for size, doc_ref in zip(sizes, doc_refs):
        for p in range(size):
            part = first + p
            for d in range(DOCS):
                source = p * PAY + d * SLOTS
                rows[pl.ds(pl.multiple_of(total * 16, 16), SLOTS), :] = doc_ref[source : source + SLOTS, :]
                for k in range(SLOTS // 16):
                    owner[total + k] = part * DOCS + d
                total = total + ((facts_ref[part * 8 + d] + 15) >> 4)
        first += size
    for k in range(SMALL):
        owner[total + k] = doc_count
    carry[...] = jnp.full_like(carry, neg_fill)

    def step(groups, base, last):
        ids = [owner[base + g] for g in range(groups)]
        drop = [jnp.where(a == b, 0.0, neg_fill) for a, b in zip(ids, [last] + ids[:-1])]
        block_rows = rows[pl.ds(pl.multiple_of(base * 16, 16), groups * 16), :]
        for b in range(blocks):
            similar = lax.dot_general(
                block_rows,
                query_ref[b * 256 : (b + 1) * 256, :],
                (((1,), (1,)), ((), ())),
                preferred_element_type=jnp.float32,
            )
            for h in range(2):
                run = carry[2 * b + h]
                for g in range(groups):
                    tile = similar[16 * g : 16 * g + 16, 128 * h : 128 * h + 128]
                    run = jnp.maximum(jnp.maximum(tile[:8], tile[8:]), run + drop[g])
                    best[2 * b + h, pl.ds(pl.multiple_of(ids[g] * 8, 8), 8), :] = run
                carry[2 * b + h] = run
        return ids[-1]

    large = total >> 6
    last = lax.fori_loop(0, large, lambda i, last: step(LARGE, i * LARGE, last), jnp.int32(-1))
    small = (total - large * LARGE + SMALL - 1) >> 4
    lax.fori_loop(0, small, lambda i, last: step(SMALL, large * LARGE + i * SMALL, last), last)

    for part in range(sum(sizes)):
        columns = []
        for half in range(2 * blocks):
            v = [best[half, (part * 8 + d) * 8 : (part * 8 + d + 1) * 8, :] for d in range(8)]
            for shift in (1, 2, 4):
                v = [merge_max(v[2 * k], v[2 * k + 1], shift) for k in range(len(v) // 2)]
            columns.append(v[0])
        for shift in (1, 2, 4, 8, 16):
            columns = [merge_sum(columns[2 * k], columns[2 * k + 1], shift) for k in range(len(columns) // 2)]
        if final:
            rest[5][doc_count + part * 8 : doc_count + part * 8 + 8, :] = columns[0]
        else:
            out_ref[part * 8 : part * 8 + 8, :] = columns[0]
    if final:
        scores, turned = rest[5:]
        me = lax.axis_index("d")
        scores[:doc_count, :] = earlier_ref[...]
        for part, source in enumerate(doc_sources(me)):
            ids = source * DOCS + lax.broadcasted_iota(jnp.int32, (8, 128), 0)
            scores[64 + part * 8 : 64 + part * 8 + 8, :] = ids.astype(jnp.float32)
        turned[...] = scores[...].T
        for b in range(blocks):
            quarters = [turned[pl.ds(2 * b + h, 4, stride=32), :] for h in range(2)]
            out_ref[block_member(me, b)] = jnp.concatenate(quarters)


def score(facts, docs, queries, earlier=None):
    sizes = [d.shape[0] // PAY for d in docs]
    doc_count = DOCS * sum(sizes)
    blocks = queries.shape[0] // 256
    final = earlier is not None
    operands = [*docs, queries] + ([earlier] if final else [])
    return pl.pallas_call(
        functools.partial(score_kernel, sizes, blocks, final),
        out_shape=pltpu.VMEM((16, 8, 128) if final else (doc_count, 128), jnp.float32),
        in_specs=[spec(pltpu.SMEM)] + [spec(pltpu.VMEM)] * len(operands),
        out_specs=spec(pltpu.VMEM),
        scratch_shapes=[
            pltpu.VMEM((doc_count * SLOTS + SMALL * 16, DIM), jnp.bfloat16),
            pltpu.VMEM((blocks * 2, (doc_count + 1) * 8, 128), jnp.float32),
            pltpu.SMEM((doc_count * 8 + SMALL,), jnp.int32),
            pltpu.VMEM((blocks * 2, 8, 128), jnp.float32),
        ]
        + ([pltpu.VMEM((128, 128), jnp.float32)] * 2 if final else []),
        compiler_params=pltpu.CompilerParams(vmem_limit_bytes=24 * 2**20),
        cost_estimate=pl.CostEstimate(flops=6 * 10**9, bytes_accessed=10**6, transcendentals=0),
        name="score",
    )(facts, *operands)


def lengths_of(docs):
    facts = [d[(k + 1) * PAY - 16, :DOCS] for d in docs for k in range(d.shape[0] // PAY)]
    return jnp.stack(facts).astype(jnp.int32).reshape(-1)


def finish_kernel(positives_ref, given_ref, out_ref):
    lane = lax.broadcasted_iota(jnp.int32, (8, 128), 1)
    row = lax.broadcasted_iota(jnp.int32, (8, 128), 0)
    wanted = jnp.zeros((8, 128), jnp.int32)
    for q in range(QUERIES):
        wanted = jnp.where(row == q, positives_ref[q], wanted)
    wanted = wanted.astype(jnp.float32)
    count = given_ref.shape[0]
    given = [given_ref[k] for k in range(count)]
    real = [jnp.where(lane < 64, g, neg_fill) for g in given]
    peak = jnp.max(functools.reduce(jnp.maximum, real), axis=1, keepdims=True)
    total = jnp.sum(sum(jnp.where(lane < 64, jnp.exp(r - peak), 0.0) for r in real), axis=1, keepdims=True)
    chosen = [jnp.where((lane < 64) & (pltpu.roll(g, 64, 1) == wanted), g, 0.0) for g in given]
    loss = peak + jnp.log(total) - jnp.sum(sum(chosen), axis=1, keepdims=True)
    out_ref[...] = jnp.sum(jnp.where(row == lane, loss, 0.0), axis=0)[:QUERIES]


def finish(positives, given):
    return pl.pallas_call(
        finish_kernel,
        out_shape=jax.ShapeDtypeStruct((QUERIES,), jnp.float32),
        in_specs=[spec(pltpu.SMEM), spec(pltpu.VMEM)],
        out_specs=spec(pltpu.VMEM),
        name="finish",
    )(positives, given)


def local(queries, documents, lengths, positives):
    own = pack_docs(lengths, documents)
    query = queries.reshape(QUERIES * TOKENS, DIM)
    near = swap(own, DOC_STEPS, 0)
    for at in range(3):
        query = jnp.concatenate([query, swap(query, QUERY_STEPS, at)])
    query = jnp.concatenate([query, swap_cores(query)])
    both = jnp.concatenate([own, near])
    far = swap(both, DOC_STEPS, 1)
    docs = [both, far], [swap(both, DOC_STEPS, 2), swap(far, DOC_STEPS, 2)]
    given = score(lengths_of(docs[0]), docs[0], query)
    given = score(lengths_of(docs[1]), docs[1], query, given)
    given = lax.all_to_all(given, "d", 0, 0, tiled=True, axis_index_groups=owner_groups())
    return finish(positives, given)


def solution(mesh):
    flat = Mesh(mesh.devices.reshape(-1), ("d",))
    placed = P("d")
    return jax.shard_map(local, mesh=flat, in_specs=(placed,) * 4, out_specs=placed, check_vma=False)
```

```python
import functools

import jax
import jax.numpy as jnp
from jax import lax
from jax.experimental import pallas as pl
from jax.experimental.pallas import tpu as pltpu
from jax.sharding import Mesh, PartitionSpec as P


neg_fill = -1e30
QUERIES, TOKENS, DOCS, SLOTS, DIM = 8, 32, 8, 128, 128
PAY = DOCS * SLOTS + 16
LARGE, SMALL = 64, 16


def index(x, y, z, core):
    return (((y // 2 * 4 + x) * 2 + core) * 2 + y % 2) * 4 + z


def everywhere():
    return [(x, y, z, c) for x in range(4) for y in range(4) for z in range(4) for c in range(2)]


def across(dim, place):
    axis = "xyz".index(dim[0])
    moved = list(place)
    moved[axis] = place[axis] ^ 1 if dim[1] == "a" else 3 - place[axis]
    return tuple(moved)


def side(dim, place):
    at = place["xyz".index(dim[0])]
    return ((0, 1, 1, 0) if dim[1] == "a" else (0, 0, 1, 1))[at]


DOC_STEPS = (("xb", "yb", "zb"), ("yb", "zb", "xb"))
QUERY_STEPS = (("xa", "ya", "za"), ("ya", "za", "xa"))


def swap(array, steps, at):
    pairs = [(index(*p), index(*across(steps[p[3]][at], p))) for p in everywhere()]
    return lax.ppermute(array, "d", pairs)


def swap_cores(array):
    pairs = [(index(x, y, z, c), index(x, y, z, 1 - c)) for x, y, z, c in everywhere()]
    return lax.ppermute(array, "d", pairs)


def member(place):
    return sum(side(dim, place) << k for k, dim in enumerate(QUERY_STEPS[place[3]]))


def member(place):
    return place[3] * 8 + sum(side(dim, place) << k for k, dim in enumerate(QUERY_STEPS[0]))


def owner_groups():
    groups = {}
    for p in everywhere():
        groups.setdefault(tuple(side(dim, p) for dim in DOC_STEPS[0]), []).append(p)
    return [[index(*p) for p in sorted(g, key=member)] for g in groups.values()]


def spec(space):
    return pl.BlockSpec(memory_space=space)


def pack_kernel(lengths_ref, docs_ref, queries_ref, out_ref, query_out):
    query_out[...] = queries_ref[...]
    row = lax.broadcasted_iota(jnp.int32, (SLOTS, DIM), 0)
    for d in range(DOCS):
        doc = docs_ref[d].astype(jnp.float32)
        doc = jnp.where(row < lengths_ref[d], doc, doc[:1, :])
        out_ref[d * SLOTS : (d + 1) * SLOTS, :] = doc.astype(jnp.bfloat16)
    lane = lax.broadcasted_iota(jnp.int32, (16, DIM), 1)
    facts = jnp.zeros((16, DIM), jnp.int32)
    for d in range(DOCS):
        facts = jnp.where(lane == d, lengths_ref[d], facts)
    out_ref[DOCS * SLOTS :, :] = facts.astype(jnp.float32).astype(jnp.bfloat16)


def pack(lengths, docs, queries):
    return pl.pallas_call(
        pack_kernel,
        out_shape=(pltpu.VMEM((PAY, DIM), jnp.bfloat16), pltpu.VMEM(queries.shape, jnp.bfloat16)),
        in_specs=[spec(pltpu.SMEM), spec(pltpu.VMEM), spec(pltpu.VMEM)],
        out_specs=(spec(pltpu.VMEM), spec(pltpu.VMEM)),
        cost_estimate=pl.CostEstimate(flops=10**6, bytes_accessed=10**6, transcendentals=0),
        name="pack",
    )(lengths, docs, queries)


def lower_half(shift, axis):
    return (lax.broadcasted_iota(jnp.int32, (8, 128), axis) // shift) % 2 == 0


def merge_max(a, b, shift):
    low = lower_half(shift, 0)
    return jnp.maximum(jnp.where(low, a, b), pltpu.roll(jnp.where(low, b, a), shift, 0))


def merge_sum(a, b, shift):
    return jnp.where(lower_half(shift, 1), a + pltpu.roll(a, 128 - shift, 1), b + pltpu.roll(b, shift, 1))


def doc_sources(me):
    flips = {"xb": 48, "yb": 68, "zb": 3}
    first, second, third = (
        jnp.where((me >> 3) & 1 == 0, flips[a], flips[b]) for a, b in zip(DOC_STEPS[0], DOC_STEPS[1])
    )
    masks = [0, first, second, first ^ second]
    return [me ^ m for m in masks] + [me ^ third ^ m for m in masks]


def block_member(me, block):
    yh, x1, x0, core, yl, z1, z0 = [(me >> k) & 1 for k in (6, 5, 4, 3, 2, 1, 0)]
    mine = (x0 ^ x1) | (yl ^ yh) << 1 | (z0 ^ z1) << 2
    flips = []
    for steps in QUERY_STEPS:
        flips.append(sum(((block >> k) & 1) << QUERY_STEPS[0].index(dim) for k, dim in enumerate(steps)))
    other = block >> 3
    return ((core ^ other) << 3) | (mine ^ jnp.where(core == other, flips[0], flips[1]))


def score_kernel(sizes, blocks, final, facts_ref, *refs):
    doc_refs, rest = refs[: len(sizes)], refs[len(sizes) :]
    query_refs, rest = rest[:2], rest[2:]
    if final:
        earlier_ref, rest = rest[0], rest[1:]
    out_ref, rows, best, owner, carry = rest[:5]
    doc_count = DOCS * sum(sizes)
    total = jnp.int32(0)
    first = 0
    for size, doc_ref in zip(sizes, doc_refs):
        for p in range(size):
            part = first + p
            for d in range(DOCS):
                source = p * PAY + d * SLOTS
                rows[pl.ds(pl.multiple_of(total * 16, 16), SLOTS), :] = doc_ref[source : source + SLOTS, :]
                for k in range(SLOTS // 16):
                    owner[total + k] = part * DOCS + d
                total = total + ((facts_ref[part * 8 + d] + 15) >> 4)
        first += size
    for k in range(SMALL):
        owner[total + k] = doc_count
    carry[...] = jnp.full_like(carry, neg_fill)

    def step(groups, base, last):
        ids = [owner[base + g] for g in range(groups)]
        drop = [jnp.where(a == b, 0.0, neg_fill) for a, b in zip(ids, [last] + ids[:-1])]
        block_rows = rows[pl.ds(pl.multiple_of(base * 16, 16), groups * 16), :]
        for b in range(blocks):
            similar = lax.dot_general(
                block_rows,
                query_refs[b // 8][b % 8 * 256 : (b % 8 + 1) * 256, :],
                (((1,), (1,)), ((), ())),
                preferred_element_type=jnp.float32,
            )
            for h in range(2):
                run = carry[2 * b + h]
                for g in range(groups):
                    tile = similar[16 * g : 16 * g + 16, 128 * h : 128 * h + 128]
                    run = jnp.maximum(jnp.maximum(tile[:8], tile[8:]), run + drop[g])
                    best[2 * b + h, pl.ds(pl.multiple_of(ids[g] * 8, 8), 8), :] = run
                carry[2 * b + h] = run
        return ids[-1]

    large = total >> 6
    last = lax.fori_loop(0, large, lambda i, last: step(LARGE, i * LARGE, last), jnp.int32(-1))
    small = (total - large * LARGE + SMALL - 1) >> 4
    lax.fori_loop(0, small, lambda i, last: step(SMALL, large * LARGE + i * SMALL, last), last)

    for part in range(sum(sizes)):
        columns = []
        for half in range(2 * blocks):
            v = [best[half, (part * 8 + d) * 8 : (part * 8 + d + 1) * 8, :] for d in range(8)]
            for shift in (1, 2, 4):
                v = [merge_max(v[2 * k], v[2 * k + 1], shift) for k in range(len(v) // 2)]
            columns.append(v[0])
        for shift in (1, 2, 4, 8, 16):
            columns = [merge_sum(columns[2 * k], columns[2 * k + 1], shift) for k in range(len(columns) // 2)]
        if final:
            rest[5][doc_count + part * 8 : doc_count + part * 8 + 8, :] = columns[0]
        else:
            out_ref[part * 8 : part * 8 + 8, :] = columns[0]
    if final:
        scores, turned = rest[5:]
        me = lax.axis_index("d")
        scores[:doc_count, :] = earlier_ref[...]
        for part, source in enumerate(doc_sources(me)):
            ids = source * DOCS + lax.broadcasted_iota(jnp.int32, (8, 128), 0)
            scores[64 + part * 8 : 64 + part * 8 + 8, :] = ids.astype(jnp.float32)
        turned[...] = scores[...].T
        for b in range(blocks):
            quarters = [turned[pl.ds(2 * b + h, 4, stride=32), :] for h in range(2)]
            out_ref[block_member(me, b)] = jnp.concatenate(quarters)


def score(facts, docs, queries, earlier=None):
    sizes = [d.shape[0] // PAY for d in docs]
    doc_count = DOCS * sum(sizes)
    blocks = sum(q.shape[0] for q in queries) // 256
    final = earlier is not None
    operands = [*docs, *queries] + ([earlier] if final else [])
    return pl.pallas_call(
        functools.partial(score_kernel, sizes, blocks, final),
        out_shape=pltpu.VMEM((16, 8, 128) if final else (doc_count, 128), jnp.float32),
        in_specs=[spec(pltpu.SMEM)] + [spec(pltpu.VMEM)] * len(operands),
        out_specs=spec(pltpu.VMEM),
        scratch_shapes=[
            pltpu.VMEM((doc_count * SLOTS + SMALL * 16, DIM), jnp.bfloat16),
            pltpu.VMEM((blocks * 2, (doc_count + 1) * 8, 128), jnp.float32),
            pltpu.SMEM((doc_count * 8 + SMALL,), jnp.int32),
            pltpu.VMEM((blocks * 2, 8, 128), jnp.float32),
        ]
        + ([pltpu.VMEM((128, 128), jnp.float32)] * 2 if final else []),
        compiler_params=pltpu.CompilerParams(vmem_limit_bytes=24 * 2**20),
        cost_estimate=pl.CostEstimate(flops=6 * 10**9, bytes_accessed=10**6, transcendentals=0),
        name="score",
    )(facts, *operands)


def lengths_of(docs):
    facts = [d[(k + 1) * PAY - 16, :DOCS] for d in docs for k in range(d.shape[0] // PAY)]
    return jnp.stack(facts).astype(jnp.int32).reshape(-1)


def finish_kernel(positives_ref, given_ref, out_ref):
    lane = lax.broadcasted_iota(jnp.int32, (8, 128), 1)
    row = lax.broadcasted_iota(jnp.int32, (8, 128), 0)
    wanted = jnp.zeros((8, 128), jnp.int32)
    for q in range(QUERIES):
        wanted = jnp.where(row == q, positives_ref[q], wanted)
    wanted = wanted.astype(jnp.float32)
    count = given_ref.shape[0]
    given = [given_ref[k] for k in range(count)]
    real = [jnp.where(lane < 64, g, neg_fill) for g in given]
    peak = jnp.max(functools.reduce(jnp.maximum, real), axis=1, keepdims=True)
    total = jnp.sum(sum(jnp.where(lane < 64, jnp.exp(r - peak), 0.0) for r in real), axis=1, keepdims=True)
    chosen = [jnp.where((lane < 64) & (pltpu.roll(g, 64, 1) == wanted), g, 0.0) for g in given]
    loss = peak + jnp.log(total) - jnp.sum(sum(chosen), axis=1, keepdims=True)
    out_ref[...] = jnp.sum(jnp.where(row == lane, loss, 0.0), axis=0)[:QUERIES]


def finish(positives, given):
    return pl.pallas_call(
        finish_kernel,
        out_shape=jax.ShapeDtypeStruct((QUERIES,), jnp.float32),
        in_specs=[spec(pltpu.SMEM), spec(pltpu.VMEM)],
        out_specs=spec(pltpu.VMEM),
        name="finish",
    )(positives, given)


def local(queries, documents, lengths, positives):
    own, query = pack(lengths, documents, queries.reshape(QUERIES * TOKENS, DIM))
    near = swap(own, DOC_STEPS, 0)
    got = swap(query, QUERY_STEPS, 0)
    query = jnp.concatenate([query, got])
    got = swap(query, QUERY_STEPS, 1)
    both = jnp.concatenate([own, near])
    far = swap(both, DOC_STEPS, 1)
    query = jnp.concatenate([query, got])
    got = swap(query, QUERY_STEPS, 2)
    third = swap(both, DOC_STEPS, 2)
    query = jnp.concatenate([query, got])
    got = swap_cores(query)
    fourth = swap(far, DOC_STEPS, 2)
    queries = [query, got]
    given = score(lengths_of([both, far]), [both, far], queries)
    given = score(lengths_of([third, fourth]), [third, fourth], queries, given)
    given = lax.all_to_all(given, "d", 0, 0, tiled=True, axis_index_groups=owner_groups())
    return finish(positives, given)


def solution(mesh):
    flat = Mesh(mesh.devices.reshape(-1), ("d",))
    placed = P("d")
    return jax.shard_map(local, mesh=flat, in_specs=(placed,) * 4, out_specs=placed, check_vma=False)
```

```python
import functools

import jax
import jax.numpy as jnp
from jax import lax
from jax.experimental import pallas as pl
from jax.experimental.pallas import tpu as pltpu
from jax.sharding import Mesh, PartitionSpec as P


neg_fill = -1e30
QUERIES, TOKENS, DOCS, SLOTS, DIM = 8, 32, 8, 128, 128
PAY = DOCS * SLOTS + 16
LARGE, SMALL = 64, 16


def index(x, y, z, core):
    return (((y // 2 * 4 + x) * 2 + core) * 2 + y % 2) * 4 + z


def everywhere():
    return [(x, y, z, c) for x in range(4) for y in range(4) for z in range(4) for c in range(2)]


def across(dim, place):
    axis = "xyz".index(dim[0])
    moved = list(place)
    moved[axis] = place[axis] ^ 1 if dim[1] == "a" else 3 - place[axis]
    return tuple(moved)


def side(dim, place):
    at = place["xyz".index(dim[0])]
    return ((0, 1, 1, 0) if dim[1] == "a" else (0, 0, 1, 1))[at]


DOC_STEPS = (("xb", "yb", "zb"), ("yb", "zb", "xb"))
QUERY_STEPS = (("xa", "ya", "za"), ("ya", "za", "xa"))


def swap(array, steps, at):
    pairs = [(index(*p), index(*across(steps[p[3]][at], p))) for p in everywhere()]
    return lax.ppermute(array, "d", pairs)


def swap_cores(array):
    pairs = [(index(x, y, z, c), index(x, y, z, 1 - c)) for x, y, z, c in everywhere()]
    return lax.ppermute(array, "d", pairs)


def member(place):
    return sum(side(dim, place) << k for k, dim in enumerate(QUERY_STEPS[place[3]]))


def member(place):
    return place[3] * 8 + sum(side(dim, place) << k for k, dim in enumerate(QUERY_STEPS[0]))


def owner_groups():
    groups = {}
    for p in everywhere():
        groups.setdefault(tuple(side(dim, p) for dim in DOC_STEPS[0]), []).append(p)
    return [[index(*p) for p in sorted(g, key=member)] for g in groups.values()]


def spec(space):
    return pl.BlockSpec(memory_space=space)


def pack_kernel(lengths_ref, docs_ref, queries_ref, out_ref, query_out):
    query_out[...] = queries_ref[...]
    row = lax.broadcasted_iota(jnp.int32, (SLOTS, DIM), 0)
    for d in range(DOCS):
        doc = docs_ref[d].astype(jnp.float32)
        doc = jnp.where(row < lengths_ref[d], doc, doc[:1, :])
        out_ref[d * SLOTS : (d + 1) * SLOTS, :] = doc.astype(jnp.bfloat16)
    lane = lax.broadcasted_iota(jnp.int32, (16, DIM), 1)
    facts = jnp.zeros((16, DIM), jnp.int32)
    for d in range(DOCS):
        facts = jnp.where(lane == d, lengths_ref[d], facts)
    out_ref[DOCS * SLOTS :, :] = facts.astype(jnp.float32).astype(jnp.bfloat16)


def pack(lengths, docs, queries):
    return pl.pallas_call(
        pack_kernel,
        out_shape=(pltpu.VMEM((PAY, DIM), jnp.bfloat16), pltpu.VMEM(queries.shape, jnp.bfloat16)),
        in_specs=[spec(pltpu.SMEM), spec(pltpu.VMEM), spec(pltpu.VMEM)],
        out_specs=(spec(pltpu.VMEM), spec(pltpu.VMEM)),
        cost_estimate=pl.CostEstimate(flops=10**6, bytes_accessed=10**6, transcendentals=0),
        name="pack",
    )(lengths, docs, queries)


def lower_half(shift, axis):
    return (lax.broadcasted_iota(jnp.int32, (8, 128), axis) // shift) % 2 == 0


def merge_max(a, b, shift):
    low = lower_half(shift, 0)
    return jnp.maximum(jnp.where(low, a, b), pltpu.roll(jnp.where(low, b, a), shift, 0))


def merge_sum(a, b, shift):
    return jnp.where(lower_half(shift, 1), a + pltpu.roll(a, 128 - shift, 1), b + pltpu.roll(b, shift, 1))


def doc_sources(me):
    flips = {"xb": 48, "yb": 68, "zb": 3}
    first, second, third = (
        jnp.where((me >> 3) & 1 == 0, flips[a], flips[b]) for a, b in zip(DOC_STEPS[0], DOC_STEPS[1])
    )
    masks = [0, first, second, first ^ second]
    return [me ^ m for m in masks] + [me ^ third ^ m for m in masks]


def block_member(me, block):
    yh, x1, x0, core, yl, z1, z0 = [(me >> k) & 1 for k in (6, 5, 4, 3, 2, 1, 0)]
    mine = (x0 ^ x1) | (yl ^ yh) << 1 | (z0 ^ z1) << 2
    flips = []
    for steps in QUERY_STEPS:
        flips.append(sum(((block >> k) & 1) << QUERY_STEPS[0].index(dim) for k, dim in enumerate(steps)))
    other = block >> 3
    return ((core ^ other) << 3) | (mine ^ jnp.where(core == other, flips[0], flips[1]))


def score_kernel(sizes, blocks, final, facts_ref, *refs):
    doc_refs, rest = refs[: len(sizes)], refs[len(sizes) :]
    query_refs, rest = rest[:2], rest[2:]
    if final:
        earlier_ref, rest = rest[0], rest[1:]
    out_ref, rows, best, owner, carry = rest[:5]
    doc_count = DOCS * sum(sizes)
    total = jnp.int32(0)
    first = 0
    for size, doc_ref in zip(sizes, doc_refs):
        for p in range(size):
            part = first + p
            for d in range(DOCS):
                source = p * PAY + d * SLOTS
                rows[pl.ds(pl.multiple_of(total * 16, 16), SLOTS), :] = doc_ref[source : source + SLOTS, :]
                for k in range(SLOTS // 16):
                    owner[total + k] = part * DOCS + d
                total = total + ((facts_ref[part * 8 + d] + 15) >> 4)
        first += size
    for k in range(SMALL):
        owner[total + k] = doc_count
    carry[...] = jnp.full_like(carry, neg_fill)

    def step(groups, base, last):
        ids = [owner[base + g] for g in range(groups)]
        drop = [jnp.where(a == b, 0.0, neg_fill) for a, b in zip(ids, [last] + ids[:-1])]
        block_rows = rows[pl.ds(pl.multiple_of(base * 16, 16), groups * 16), :]
        for b in range(blocks):
            similar = lax.dot_general(
                block_rows,
                query_refs[b // 8][b % 8 * 256 : (b % 8 + 1) * 256, :],
                (((1,), (1,)), ((), ())),
                preferred_element_type=jnp.float32,
            )
            for h in range(2):
                run = carry[2 * b + h]
                for g in range(groups):
                    tile = similar[16 * g : 16 * g + 16, 128 * h : 128 * h + 128]
                    run = jnp.maximum(jnp.maximum(tile[:8], tile[8:]), run + drop[g])
                    best[2 * b + h, pl.ds(pl.multiple_of(ids[g] * 8, 8), 8), :] = run
                carry[2 * b + h] = run
        return ids[-1]

    large = total >> 6
    last = lax.fori_loop(0, large, lambda i, last: step(LARGE, i * LARGE, last), jnp.int32(-1))
    small = (total - large * LARGE + SMALL - 1) >> 4
    lax.fori_loop(0, small, lambda i, last: step(SMALL, large * LARGE + i * SMALL, last), last)

    for part in range(sum(sizes)):
        columns = []
        for half in range(2 * blocks):
            v = [best[half, (part * 8 + d) * 8 : (part * 8 + d + 1) * 8, :] for d in range(8)]
            for shift in (1, 2, 4):
                v = [merge_max(v[2 * k], v[2 * k + 1], shift) for k in range(len(v) // 2)]
            columns.append(v[0])
        for shift in (1, 2, 4, 8, 16):
            columns = [merge_sum(columns[2 * k], columns[2 * k + 1], shift) for k in range(len(columns) // 2)]
        if final:
            rest[5][doc_count + part * 8 : doc_count + part * 8 + 8, :] = columns[0]
        else:
            out_ref[part * 8 : part * 8 + 8, :] = columns[0]
    if final:
        scores, turned = rest[5:]
        me = lax.axis_index("d")
        scores[:doc_count, :] = earlier_ref[...]
        for part, source in enumerate(doc_sources(me)):
            ids = source * DOCS + lax.broadcasted_iota(jnp.int32, (8, 128), 0)
            scores[64 + part * 8 : 64 + part * 8 + 8, :] = ids.astype(jnp.float32)
        turned[...] = scores[...].T
        for b in range(blocks):
            quarters = [turned[pl.ds(2 * b + h, 4, stride=32), :] for h in range(2)]
            out_ref[block_member(me, b)] = jnp.concatenate(quarters)


def score(facts, docs, queries, earlier=None):
    sizes = [d.shape[0] // PAY for d in docs]
    doc_count = DOCS * sum(sizes)
    blocks = sum(q.shape[0] for q in queries) // 256
    final = earlier is not None
    operands = [*docs, *queries] + ([earlier] if final else [])
    return pl.pallas_call(
        functools.partial(score_kernel, sizes, blocks, final),
        out_shape=pltpu.VMEM((16, 8, 128) if final else (doc_count, 128), jnp.float32),
        in_specs=[spec(pltpu.SMEM)] + [spec(pltpu.VMEM)] * len(operands),
        out_specs=spec(pltpu.VMEM),
        scratch_shapes=[
            pltpu.VMEM((doc_count * SLOTS + SMALL * 16, DIM), jnp.bfloat16),
            pltpu.VMEM((blocks * 2, (doc_count + 1) * 8, 128), jnp.float32),
            pltpu.SMEM((doc_count * 8 + SMALL,), jnp.int32),
            pltpu.VMEM((blocks * 2, 8, 128), jnp.float32),
        ]
        + ([pltpu.VMEM((128, 128), jnp.float32)] * 2 if final else []),
        compiler_params=pltpu.CompilerParams(vmem_limit_bytes=24 * 2**20),
        cost_estimate=pl.CostEstimate(flops=6 * 10**9, bytes_accessed=10**6, transcendentals=0),
        name="score",
    )(facts, *operands)


def lengths_of(docs):
    facts = [d[(k + 1) * PAY - 16, :DOCS] for d in docs for k in range(d.shape[0] // PAY)]
    return jnp.stack(facts).astype(jnp.int32).reshape(-1)


def finish_kernel(positives_ref, given_ref, out_ref):
    lane = lax.broadcasted_iota(jnp.int32, (8, 128), 1)
    row = lax.broadcasted_iota(jnp.int32, (8, 128), 0)
    wanted = jnp.zeros((8, 128), jnp.int32)
    for q in range(QUERIES):
        wanted = jnp.where(row == q, positives_ref[q], wanted)
    wanted = wanted.astype(jnp.float32)
    count = given_ref.shape[0]
    given = [given_ref[k] for k in range(count)]
    real = [jnp.where(lane < 64, g, neg_fill) for g in given]
    peak = jnp.max(functools.reduce(jnp.maximum, real), axis=1, keepdims=True)
    total = jnp.sum(sum(jnp.where(lane < 64, jnp.exp(r - peak), 0.0) for r in real), axis=1, keepdims=True)
    chosen = [jnp.where((lane < 64) & (pltpu.roll(g, 64, 1) == wanted), g, 0.0) for g in given]
    loss = peak + jnp.log(total) - jnp.sum(sum(chosen), axis=1, keepdims=True)
    out_ref[...] = jnp.sum(jnp.where(row == lane, loss, 0.0), axis=0)[:QUERIES]


def finish(positives, given):
    return pl.pallas_call(
        finish_kernel,
        out_shape=jax.ShapeDtypeStruct((QUERIES,), jnp.float32),
        in_specs=[spec(pltpu.SMEM), spec(pltpu.VMEM)],
        out_specs=spec(pltpu.VMEM),
        name="finish",
    )(positives, given)


def local(queries, documents, lengths, positives):
    query = queries.reshape(QUERIES * TOKENS, DIM)
    got = swap(query, QUERY_STEPS, 0)
    own, query = pack(lengths, documents, query)
    first = swap(own, DOC_STEPS, 0)
    second = swap(own, DOC_STEPS, 1)
    query = jnp.concatenate([query, got])
    query = jnp.concatenate([query, swap(query, QUERY_STEPS, 1)])
    query = jnp.concatenate([query, swap(query, QUERY_STEPS, 2)])
    near = [own, first, second, swap(first, DOC_STEPS, 1)]
    far = [swap(jnp.concatenate(near[:2]), DOC_STEPS, 2), swap(jnp.concatenate(near[2:]), DOC_STEPS, 2)]
    queries = [query, swap_cores(query)]
    given = score(lengths_of(near), near, queries)
    given = score(lengths_of(far), far, queries, given)
    given = lax.all_to_all(given, "d", 0, 0, tiled=True, axis_index_groups=owner_groups())
    return finish(positives, given)


def solution(mesh):
    flat = Mesh(mesh.devices.reshape(-1), ("d",))
    placed = P("d")
    return jax.shard_map(local, mesh=flat, in_specs=(placed,) * 4, out_specs=placed, check_vma=False)
```

```python
import functools

import jax
import jax.numpy as jnp
from jax import lax
from jax.experimental import pallas as pl
from jax.experimental.pallas import tpu as pltpu
from jax.sharding import Mesh, PartitionSpec as P


neg_fill = -1e30
QUERIES, TOKENS, DOCS, SLOTS, DIM = 8, 32, 8, 128, 128
PAY = DOCS * SLOTS + 16
STEPS = (64, 32, 16)


def index(x, y, z, core):
    return (((y // 2 * 4 + x) * 2 + core) * 2 + y % 2) * 4 + z


def everywhere():
    return [(x, y, z, c) for x in range(4) for y in range(4) for z in range(4) for c in range(2)]


def across(dim, place):
    axis = "xyz".index(dim[0])
    moved = list(place)
    moved[axis] = place[axis] ^ 1 if dim[1] == "a" else 3 - place[axis]
    return tuple(moved)


def side(dim, place):
    at = place["xyz".index(dim[0])]
    return ((0, 1, 1, 0) if dim[1] == "a" else (0, 0, 1, 1))[at]


DOC_STEPS = (("xb", "yb", "zb"), ("yb", "zb", "xb"))
QUERY_STEPS = (("xa", "ya", "za"), ("ya", "za", "xa"))


def swap(array, steps, at):
    pairs = [(index(*p), index(*across(steps[p[3]][at], p))) for p in everywhere()]
    return lax.ppermute(array, "d", pairs)


def swap_cores(array):
    pairs = [(index(x, y, z, c), index(x, y, z, 1 - c)) for x, y, z, c in everywhere()]
    return lax.ppermute(array, "d", pairs)


def member(place):
    return sum(side(dim, place) << k for k, dim in enumerate(QUERY_STEPS[place[3]]))


def member(place):
    return place[3] * 8 + sum(side(dim, place) << k for k, dim in enumerate(QUERY_STEPS[0]))


def owner_groups():
    groups = {}
    for p in everywhere():
        groups.setdefault(tuple(side(dim, p) for dim in DOC_STEPS[0]), []).append(p)
    return [[index(*p) for p in sorted(g, key=member)] for g in groups.values()]


def spec(space):
    return pl.BlockSpec(memory_space=space)


def pack_kernel(lengths_ref, docs_ref, queries_ref, out_ref, query_out):
    query_out[...] = queries_ref[...]
    row = lax.broadcasted_iota(jnp.int32, (SLOTS, DIM), 0)
    for d in range(DOCS):
        doc = docs_ref[d].astype(jnp.float32)
        doc = jnp.where(row < lengths_ref[d], doc, doc[:1, :])
        out_ref[d * SLOTS : (d + 1) * SLOTS, :] = doc.astype(jnp.bfloat16)
    lane = lax.broadcasted_iota(jnp.int32, (16, DIM), 1)
    facts = jnp.zeros((16, DIM), jnp.int32)
    for d in range(DOCS):
        facts = jnp.where(lane == d, lengths_ref[d], facts)
    out_ref[DOCS * SLOTS :, :] = facts.astype(jnp.float32).astype(jnp.bfloat16)


def pack(lengths, docs, queries):
    return pl.pallas_call(
        pack_kernel,
        out_shape=(pltpu.VMEM((PAY, DIM), jnp.bfloat16), pltpu.VMEM(queries.shape, jnp.bfloat16)),
        in_specs=[spec(pltpu.SMEM), spec(pltpu.VMEM), spec(pltpu.VMEM)],
        out_specs=(spec(pltpu.VMEM), spec(pltpu.VMEM)),
        cost_estimate=pl.CostEstimate(flops=10**6, bytes_accessed=10**6, transcendentals=0),
        name="pack",
    )(lengths, docs, queries)


def lower_half(shift, axis):
    return (lax.broadcasted_iota(jnp.int32, (8, 128), axis) // shift) % 2 == 0


def merge_max(a, b, shift):
    low = lower_half(shift, 0)
    return jnp.maximum(jnp.where(low, a, b), pltpu.roll(jnp.where(low, b, a), shift, 0))


def merge_sum(a, b, shift):
    return jnp.where(lower_half(shift, 1), a + pltpu.roll(a, 128 - shift, 1), b + pltpu.roll(b, shift, 1))


def doc_sources(me):
    flips = {"xb": 48, "yb": 68, "zb": 3}
    first, second, third = (
        jnp.where((me >> 3) & 1 == 0, flips[a], flips[b]) for a, b in zip(DOC_STEPS[0], DOC_STEPS[1])
    )
    masks = [0, first, second, first ^ second]
    return [me ^ m for m in masks] + [me ^ third ^ m for m in masks]


def block_member(me, block):
    yh, x1, x0, core, yl, z1, z0 = [(me >> k) & 1 for k in (6, 5, 4, 3, 2, 1, 0)]
    mine = (x0 ^ x1) | (yl ^ yh) << 1 | (z0 ^ z1) << 2
    flips = []
    for steps in QUERY_STEPS:
        flips.append(sum(((block >> k) & 1) << QUERY_STEPS[0].index(dim) for k, dim in enumerate(steps)))
    other = block >> 3
    return ((core ^ other) << 3) | (mine ^ jnp.where(core == other, flips[0], flips[1]))


def score_kernel(sizes, blocks, final, facts_ref, *refs):
    doc_refs, rest = refs[: len(sizes)], refs[len(sizes) :]
    query_refs, rest = rest[:2], rest[2:]
    if final:
        earlier_ref, rest = rest[0], rest[1:]
    out_ref, rows, best, owner, carry = rest[:5]
    doc_count = DOCS * sum(sizes)
    total = jnp.int32(0)
    first = 0
    for size, doc_ref in zip(sizes, doc_refs):
        for p in range(size):
            part = first + p
            for d in range(DOCS):
                source = p * PAY + d * SLOTS
                rows[pl.ds(pl.multiple_of(total * 16, 16), SLOTS), :] = doc_ref[source : source + SLOTS, :]
                for k in range(SLOTS // 16):
                    owner[total + k] = part * DOCS + d
                total = total + ((facts_ref[part * 8 + d] + 15) >> 4)
        first += size
    for k in range(STEPS[-1]):
        owner[total + k] = doc_count
    carry[...] = jnp.full_like(carry, neg_fill)

    def step(groups, base, last):
        ids = [owner[base + g] for g in range(groups)]
        drop = [jnp.where(a == b, 0.0, neg_fill) for a, b in zip(ids, [last] + ids[:-1])]
        block_rows = rows[pl.ds(pl.multiple_of(base * 16, 16), groups * 16), :]
        for b in range(blocks):
            similar = lax.dot_general(
                block_rows,
                query_refs[b // 8][b % 8 * 256 : (b % 8 + 1) * 256, :],
                (((1,), (1,)), ((), ())),
                preferred_element_type=jnp.float32,
            )
            for h in range(2):
                run = carry[2 * b + h]
                for g in range(groups):
                    tile = similar[16 * g : 16 * g + 16, 128 * h : 128 * h + 128]
                    run = jnp.maximum(jnp.maximum(tile[:8], tile[8:]), run + drop[g])
                    best[2 * b + h, pl.ds(pl.multiple_of(ids[g] * 8, 8), 8), :] = run
                carry[2 * b + h] = run
        return ids[-1]

    base, last = jnp.int32(0), jnp.int32(-1)
    for groups in STEPS:
        up = groups - 1 if groups == STEPS[-1] else 0
        count = (total - base + up) >> (groups.bit_length() - 1)
        last = lax.fori_loop(
            0, count, lambda i, last, groups=groups, base=base: step(groups, base + i * groups, last), last
        )
        base = base + count * groups

    for part in range(sum(sizes)):
        columns = []
        for half in range(2 * blocks):
            v = [best[half, (part * 8 + d) * 8 : (part * 8 + d + 1) * 8, :] for d in range(8)]
            for shift in (1, 2, 4):
                v = [merge_max(v[2 * k], v[2 * k + 1], shift) for k in range(len(v) // 2)]
            columns.append(v[0])
        for shift in (1, 2, 4, 8, 16):
            columns = [merge_sum(columns[2 * k], columns[2 * k + 1], shift) for k in range(len(columns) // 2)]
        if final:
            rest[5][doc_count + part * 8 : doc_count + part * 8 + 8, :] = columns[0]
        else:
            out_ref[part * 8 : part * 8 + 8, :] = columns[0]
    if final:
        scores, turned = rest[5:]
        me = lax.axis_index("d")
        scores[:doc_count, :] = earlier_ref[...]
        for part, source in enumerate(doc_sources(me)):
            ids = source * DOCS + lax.broadcasted_iota(jnp.int32, (8, 128), 0)
            scores[64 + part * 8 : 64 + part * 8 + 8, :] = ids.astype(jnp.float32)
        turned[...] = scores[...].T
        for b in range(blocks):
            quarters = [turned[pl.ds(2 * b + h, 4, stride=32), :] for h in range(2)]
            out_ref[block_member(me, b)] = jnp.concatenate(quarters)


def score(facts, docs, queries, earlier=None):
    sizes = [d.shape[0] // PAY for d in docs]
    doc_count = DOCS * sum(sizes)
    blocks = sum(q.shape[0] for q in queries) // 256
    final = earlier is not None
    operands = [*docs, *queries] + ([earlier] if final else [])
    return pl.pallas_call(
        functools.partial(score_kernel, sizes, blocks, final),
        out_shape=pltpu.VMEM((16, 8, 128) if final else (doc_count, 128), jnp.float32),
        in_specs=[spec(pltpu.SMEM)] + [spec(pltpu.VMEM)] * len(operands),
        out_specs=spec(pltpu.VMEM),
        scratch_shapes=[
            pltpu.VMEM((doc_count * SLOTS + STEPS[-1] * 16, DIM), jnp.bfloat16),
            pltpu.VMEM((blocks * 2, (doc_count + 1) * 8, 128), jnp.float32),
            pltpu.SMEM((doc_count * 8 + STEPS[-1],), jnp.int32),
            pltpu.VMEM((blocks * 2, 8, 128), jnp.float32),
        ]
        + ([pltpu.VMEM((128, 128), jnp.float32)] * 2 if final else []),
        compiler_params=pltpu.CompilerParams(vmem_limit_bytes=24 * 2**20),
        cost_estimate=pl.CostEstimate(flops=6 * 10**9, bytes_accessed=10**6, transcendentals=0),
        name="score",
    )(facts, *operands)


def lengths_of(docs):
    facts = [d[(k + 1) * PAY - 16, :DOCS] for d in docs for k in range(d.shape[0] // PAY)]
    return jnp.stack(facts).astype(jnp.int32).reshape(-1)


def finish_kernel(positives_ref, given_ref, out_ref):
    lane = lax.broadcasted_iota(jnp.int32, (8, 128), 1)
    row = lax.broadcasted_iota(jnp.int32, (8, 128), 0)
    wanted = jnp.zeros((8, 128), jnp.int32)
    for q in range(QUERIES):
        wanted = jnp.where(row == q, positives_ref[q], wanted)
    wanted = wanted.astype(jnp.float32)
    count = given_ref.shape[0]
    given = [given_ref[k] for k in range(count)]
    real = [jnp.where(lane < 64, g, neg_fill) for g in given]
    peak = jnp.max(functools.reduce(jnp.maximum, real), axis=1, keepdims=True)
    total = jnp.sum(sum(jnp.where(lane < 64, jnp.exp(r - peak), 0.0) for r in real), axis=1, keepdims=True)
    chosen = [jnp.where((lane < 64) & (pltpu.roll(g, 64, 1) == wanted), g, 0.0) for g in given]
    loss = peak + jnp.log(total) - jnp.sum(sum(chosen), axis=1, keepdims=True)
    out_ref[...] = jnp.sum(jnp.where(row == lane, loss, 0.0), axis=0)[:QUERIES]


def finish(positives, given):
    return pl.pallas_call(
        finish_kernel,
        out_shape=jax.ShapeDtypeStruct((QUERIES,), jnp.float32),
        in_specs=[spec(pltpu.SMEM), spec(pltpu.VMEM)],
        out_specs=spec(pltpu.VMEM),
        name="finish",
    )(positives, given)


def local(queries, documents, lengths, positives):
    query = queries.reshape(QUERIES * TOKENS, DIM)
    got = swap(query, QUERY_STEPS, 0)
    own, query = pack(lengths, documents, query)
    first = swap(own, DOC_STEPS, 0)
    second = swap(own, DOC_STEPS, 1)
    query = jnp.concatenate([query, got])
    query = jnp.concatenate([query, swap(query, QUERY_STEPS, 1)])
    query = jnp.concatenate([query, swap(query, QUERY_STEPS, 2)])
    near = [own, first, second, swap(first, DOC_STEPS, 1)]
    far = [swap(jnp.concatenate(near[:3]), DOC_STEPS, 2), swap(near[3], DOC_STEPS, 2)]
    queries = [query, swap_cores(query)]
    given = score(lengths_of(near), near, queries)
    given = score(lengths_of(far), far, queries, given)
    given = lax.all_to_all(given, "d", 0, 0, tiled=True, axis_index_groups=owner_groups())
    return finish(positives, given)


def solution(mesh):
    flat = Mesh(mesh.devices.reshape(-1), ("d",))
    placed = P("d")
    return jax.shard_map(local, mesh=flat, in_specs=(placed,) * 4, out_specs=placed, check_vma=False)
```

```python
import functools

import jax
import jax.numpy as jnp
from jax import lax
from jax.experimental import pallas as pl
from jax.experimental.pallas import tpu as pltpu
from jax.sharding import Mesh, PartitionSpec as P


neg_fill = -1e30
QUERIES, TOKENS, DOCS, SLOTS, DIM = 8, 32, 8, 128, 128
PAY = DOCS * SLOTS + 16
STEPS = (64, 16)


def index(x, y, z, core):
    return (((y // 2 * 4 + x) * 2 + core) * 2 + y % 2) * 4 + z


def everywhere():
    return [(x, y, z, c) for x in range(4) for y in range(4) for z in range(4) for c in range(2)]


def across(dim, place):
    axis = "xyz".index(dim[0])
    moved = list(place)
    moved[axis] = place[axis] ^ 1 if dim[1] == "a" else 3 - place[axis]
    return tuple(moved)


def side(dim, place):
    at = place["xyz".index(dim[0])]
    return ((0, 1, 1, 0) if dim[1] == "a" else (0, 0, 1, 1))[at]


DOC_STEPS = (("xb", "yb", "zb"), ("yb", "zb", "xb"))
QUERY_STEPS = (("xa", "ya", "za"), ("ya", "za", "xa"))


def swap(array, steps, at):
    pairs = [(index(*p), index(*across(steps[p[3]][at], p))) for p in everywhere()]
    return lax.ppermute(array, "d", pairs)


def swap_cores(array):
    pairs = [(index(x, y, z, c), index(x, y, z, 1 - c)) for x, y, z, c in everywhere()]
    return lax.ppermute(array, "d", pairs)


def member(place):
    return sum(side(dim, place) << k for k, dim in enumerate(QUERY_STEPS[place[3]]))


def member(place):
    return place[3] * 8 + sum(side(dim, place) << k for k, dim in enumerate(QUERY_STEPS[0]))


def owner_groups():
    groups = {}
    for p in everywhere():
        groups.setdefault(tuple(side(dim, p) for dim in DOC_STEPS[0]), []).append(p)
    return [[index(*p) for p in sorted(g, key=member)] for g in groups.values()]


def spec(space):
    return pl.BlockSpec(memory_space=space)


def pack_kernel(lengths_ref, docs_ref, queries_ref, out_ref, query_out):
    query_out[...] = queries_ref[...]
    row = lax.broadcasted_iota(jnp.int32, (SLOTS, DIM), 0)
    for d in range(DOCS):
        doc = docs_ref[d].astype(jnp.float32)
        doc = jnp.where(row < lengths_ref[d], doc, doc[:1, :])
        out_ref[d * SLOTS : (d + 1) * SLOTS, :] = doc.astype(jnp.bfloat16)
    lane = lax.broadcasted_iota(jnp.int32, (16, DIM), 1)
    facts = jnp.zeros((16, DIM), jnp.int32)
    for d in range(DOCS):
        facts = jnp.where(lane == d, lengths_ref[d], facts)
    out_ref[DOCS * SLOTS :, :] = facts.astype(jnp.float32).astype(jnp.bfloat16)


def pack(lengths, docs, queries):
    return pl.pallas_call(
        pack_kernel,
        out_shape=(pltpu.VMEM((PAY, DIM), jnp.bfloat16), pltpu.VMEM(queries.shape, jnp.bfloat16)),
        in_specs=[spec(pltpu.SMEM), spec(pltpu.VMEM), spec(pltpu.VMEM)],
        out_specs=(spec(pltpu.VMEM), spec(pltpu.VMEM)),
        cost_estimate=pl.CostEstimate(flops=10**6, bytes_accessed=10**6, transcendentals=0),
        name="pack",
    )(lengths, docs, queries)


def join_kernel(a_ref, b_ref, out_ref):
    count = a_ref.shape[0]
    out_ref[:count, :] = a_ref[...]
    out_ref[count:, :] = b_ref[...]


def join(a, b):
    return pl.pallas_call(
        join_kernel,
        out_shape=pltpu.VMEM((a.shape[0] + b.shape[0], DIM), jnp.bfloat16),
        in_specs=[spec(pltpu.VMEM), spec(pltpu.VMEM)],
        out_specs=spec(pltpu.VMEM),
        cost_estimate=pl.CostEstimate(flops=10**6, bytes_accessed=10**6, transcendentals=0),
        name="join",
    )(a, b)


def lower_half(shift, axis):
    return (lax.broadcasted_iota(jnp.int32, (8, 128), axis) // shift) % 2 == 0


def merge_max(a, b, shift):
    low = lower_half(shift, 0)
    return jnp.maximum(jnp.where(low, a, b), pltpu.roll(jnp.where(low, b, a), shift, 0))


def merge_sum(a, b, shift):
    return jnp.where(lower_half(shift, 1), a + pltpu.roll(a, 128 - shift, 1), b + pltpu.roll(b, shift, 1))


def doc_sources(me):
    flips = {"xb": 48, "yb": 68, "zb": 3}
    first, second, third = (
        jnp.where((me >> 3) & 1 == 0, flips[a], flips[b]) for a, b in zip(DOC_STEPS[0], DOC_STEPS[1])
    )
    masks = [0, first, second, first ^ second]
    return [me ^ m for m in masks] + [me ^ third ^ m for m in masks]


def block_member(me, block):
    yh, x1, x0, core, yl, z1, z0 = [(me >> k) & 1 for k in (6, 5, 4, 3, 2, 1, 0)]
    mine = (x0 ^ x1) | (yl ^ yh) << 1 | (z0 ^ z1) << 2
    flips = []
    for steps in QUERY_STEPS:
        flips.append(sum(((block >> k) & 1) << QUERY_STEPS[0].index(dim) for k, dim in enumerate(steps)))
    other = block >> 3
    return ((core ^ other) << 3) | (mine ^ jnp.where(core == other, flips[0], flips[1]))


def score_kernel(sizes, blocks, final, facts_ref, *refs):
    doc_refs, rest = refs[: len(sizes)], refs[len(sizes) :]
    query_refs, rest = rest[:2], rest[2:]
    if final:
        earlier_ref, rest = rest[0], rest[1:]
    out_ref, rows, best, owner, carry = rest[:5]
    doc_count = DOCS * sum(sizes)
    total = jnp.int32(0)
    first = 0
    for size, doc_ref in zip(sizes, doc_refs):
        for p in range(size):
            part = first + p
            for d in range(DOCS):
                source = p * PAY + d * SLOTS
                rows[pl.ds(pl.multiple_of(total * 16, 16), SLOTS), :] = doc_ref[source : source + SLOTS, :]
                for k in range(SLOTS // 16):
                    owner[total + k] = part * DOCS + d
                total = total + ((facts_ref[part * 8 + d] + 15) >> 4)
        first += size
    for k in range(STEPS[-1]):
        owner[total + k] = doc_count
    carry[...] = jnp.full_like(carry, neg_fill)

    def step(groups, base, last):
        ids = [owner[base + g] for g in range(groups)]
        drop = [jnp.where(a == b, 0.0, neg_fill) for a, b in zip(ids, [last] + ids[:-1])]
        block_rows = rows[pl.ds(pl.multiple_of(base * 16, 16), groups * 16), :]
        for b in range(blocks):
            similar = lax.dot_general(
                block_rows,
                query_refs[b // 8][b % 8 * 256 : (b % 8 + 1) * 256, :],
                (((1,), (1,)), ((), ())),
                preferred_element_type=jnp.float32,
            )
            for h in range(2):
                run = carry[2 * b + h]
                for g in range(groups):
                    tile = similar[16 * g : 16 * g + 16, 128 * h : 128 * h + 128]
                    run = jnp.maximum(jnp.maximum(tile[:8], tile[8:]), run + drop[g])
                    best[2 * b + h, pl.ds(pl.multiple_of(ids[g] * 8, 8), 8), :] = run
                carry[2 * b + h] = run
        return ids[-1]

    base, last = jnp.int32(0), jnp.int32(-1)
    for groups in STEPS:
        up = groups - 1 if groups == STEPS[-1] else 0
        count = (total - base + up) >> (groups.bit_length() - 1)
        last = lax.fori_loop(
            0, count, lambda i, last, groups=groups, base=base: step(groups, base + i * groups, last), last
        )
        base = base + count * groups

    for part in range(sum(sizes)):
        columns = []
        for half in range(2 * blocks):
            v = [best[half, (part * 8 + d) * 8 : (part * 8 + d + 1) * 8, :] for d in range(8)]
            for shift in (1, 2, 4):
                v = [merge_max(v[2 * k], v[2 * k + 1], shift) for k in range(len(v) // 2)]
            columns.append(v[0])
        for shift in (1, 2, 4, 8, 16):
            columns = [merge_sum(columns[2 * k], columns[2 * k + 1], shift) for k in range(len(columns) // 2)]
        if final:
            rest[5][doc_count + part * 8 : doc_count + part * 8 + 8, :] = columns[0]
        else:
            out_ref[part * 8 : part * 8 + 8, :] = columns[0]
    if final:
        scores, turned = rest[5:]
        me = lax.axis_index("d")
        scores[:doc_count, :] = earlier_ref[...]
        for part, source in enumerate(doc_sources(me)):
            ids = source * DOCS + lax.broadcasted_iota(jnp.int32, (8, 128), 0)
            scores[64 + part * 8 : 64 + part * 8 + 8, :] = ids.astype(jnp.float32)
        turned[...] = scores[...].T
        for b in range(blocks):
            quarters = [turned[pl.ds(2 * b + h, 4, stride=32), :] for h in range(2)]
            out_ref[block_member(me, b)] = jnp.concatenate(quarters)


def score(facts, docs, queries, earlier=None):
    sizes = [d.shape[0] // PAY for d in docs]
    doc_count = DOCS * sum(sizes)
    blocks = sum(q.shape[0] for q in queries) // 256
    final = earlier is not None
    operands = [*docs, *queries] + ([earlier] if final else [])
    return pl.pallas_call(
        functools.partial(score_kernel, sizes, blocks, final),
        out_shape=pltpu.VMEM((16, 8, 128) if final else (doc_count, 128), jnp.float32),
        in_specs=[spec(pltpu.SMEM)] + [spec(pltpu.VMEM)] * len(operands),
        out_specs=spec(pltpu.VMEM),
        scratch_shapes=[
            pltpu.VMEM((doc_count * SLOTS + STEPS[-1] * 16, DIM), jnp.bfloat16),
            pltpu.VMEM((blocks * 2, (doc_count + 1) * 8, 128), jnp.float32),
            pltpu.SMEM((doc_count * 8 + STEPS[-1],), jnp.int32),
            pltpu.VMEM((blocks * 2, 8, 128), jnp.float32),
        ]
        + ([pltpu.VMEM((128, 128), jnp.float32)] * 2 if final else []),
        compiler_params=pltpu.CompilerParams(vmem_limit_bytes=24 * 2**20),
        cost_estimate=pl.CostEstimate(flops=6 * 10**9, bytes_accessed=10**6, transcendentals=0),
        name="score",
    )(facts, *operands)


def lengths_of(docs):
    facts = [d[(k + 1) * PAY - 16, :DOCS] for d in docs for k in range(d.shape[0] // PAY)]
    return jnp.stack(facts).astype(jnp.int32).reshape(-1)


def finish_kernel(positives_ref, given_ref, out_ref):
    lane = lax.broadcasted_iota(jnp.int32, (8, 128), 1)
    row = lax.broadcasted_iota(jnp.int32, (8, 128), 0)
    wanted = jnp.zeros((8, 128), jnp.int32)
    for q in range(QUERIES):
        wanted = jnp.where(row == q, positives_ref[q], wanted)
    wanted = wanted.astype(jnp.float32)
    count = given_ref.shape[0]
    given = [given_ref[k] for k in range(count)]
    real = [jnp.where(lane < 64, g, neg_fill) for g in given]
    peak = jnp.max(functools.reduce(jnp.maximum, real), axis=1, keepdims=True)
    total = jnp.sum(sum(jnp.where(lane < 64, jnp.exp(r - peak), 0.0) for r in real), axis=1, keepdims=True)
    chosen = [jnp.where((lane < 64) & (pltpu.roll(g, 64, 1) == wanted), g, 0.0) for g in given]
    loss = peak + jnp.log(total) - jnp.sum(sum(chosen), axis=1, keepdims=True)
    out_ref[...] = jnp.sum(jnp.where(row == lane, loss, 0.0), axis=0)[:QUERIES]


def finish(positives, given):
    return pl.pallas_call(
        finish_kernel,
        out_shape=jax.ShapeDtypeStruct((QUERIES,), jnp.float32),
        in_specs=[spec(pltpu.SMEM), spec(pltpu.VMEM)],
        out_specs=spec(pltpu.VMEM),
        name="finish",
    )(positives, given)


def local(queries, documents, lengths, positives):
    query = queries.reshape(QUERIES * TOKENS, DIM)
    got = swap(query, QUERY_STEPS, 0)
    own, query = pack(lengths, documents, query)
    first = swap(own, DOC_STEPS, 0)
    second = swap(own, DOC_STEPS, 1)
    third = swap(own, DOC_STEPS, 2)
    query = jnp.concatenate([query, got])
    query = jnp.concatenate([query, swap(query, QUERY_STEPS, 1)])
    query = jnp.concatenate([query, swap(query, QUERY_STEPS, 2)])
    near = [own, first, second, swap(first, DOC_STEPS, 1)]
    far = [third, swap(join(first, second), DOC_STEPS, 2), swap(near[3], DOC_STEPS, 2)]
    queries = [query, swap_cores(query)]
    given = score(lengths_of(near), near, queries)
    given = score(lengths_of(far), far, queries, given)
    given = lax.all_to_all(given, "d", 0, 0, tiled=True, axis_index_groups=owner_groups())
    return finish(positives, given)


def solution(mesh):
    flat = Mesh(mesh.devices.reshape(-1), ("d",))
    placed = P("d")
    return jax.shard_map(local, mesh=flat, in_specs=(placed,) * 4, out_specs=placed, check_vma=False)
```

```python
import functools

import jax
import jax.numpy as jnp
from jax import lax
from jax.experimental import pallas as pl
from jax.experimental.pallas import tpu as pltpu
from jax.sharding import Mesh, PartitionSpec as P


neg_fill = -1e30
QUERIES, TOKENS, DOCS, SLOTS, DIM = 8, 32, 8, 128, 128
PAY = DOCS * SLOTS + 16
STEPS = (64, 16)


def index(x, y, z, core):
    return (((y // 2 * 4 + x) * 2 + core) * 2 + y % 2) * 4 + z


def everywhere():
    return [(x, y, z, c) for x in range(4) for y in range(4) for z in range(4) for c in range(2)]


def across(dim, place):
    axis = "xyz".index(dim[0])
    moved = list(place)
    moved[axis] = place[axis] ^ 1 if dim[1] == "a" else 3 - place[axis]
    return tuple(moved)


def side(dim, place):
    at = place["xyz".index(dim[0])]
    return ((0, 1, 1, 0) if dim[1] == "a" else (0, 0, 1, 1))[at]


DOC_STEPS = (("zb", "yb", "xb"), ("xb", "zb", "yb"))
QUERY_STEPS = (("xa", "ya", "za"), ("ya", "za", "xa"))


def swap(array, steps, at):
    pairs = [(index(*p), index(*across(steps[p[3]][at], p))) for p in everywhere()]
    return lax.ppermute(array, "d", pairs)


def swap_cores(array):
    pairs = [(index(x, y, z, c), index(x, y, z, 1 - c)) for x, y, z, c in everywhere()]
    return lax.ppermute(array, "d", pairs)


def member(place):
    return sum(side(dim, place) << k for k, dim in enumerate(QUERY_STEPS[place[3]]))


def member(place):
    return place[3] * 8 + sum(side(dim, place) << k for k, dim in enumerate(QUERY_STEPS[0]))


def owner_groups():
    groups = {}
    for p in everywhere():
        groups.setdefault(tuple(side(dim, p) for dim in DOC_STEPS[0]), []).append(p)
    return [[index(*p) for p in sorted(g, key=member)] for g in groups.values()]


def spec(space):
    return pl.BlockSpec(memory_space=space)


def pack_kernel(lengths_ref, docs_ref, queries_ref, out_ref, query_out):
    query_out[...] = queries_ref[...]
    row = lax.broadcasted_iota(jnp.int32, (SLOTS, DIM), 0)
    for d in range(DOCS):
        doc = docs_ref[d].astype(jnp.float32)
        doc = jnp.where(row < lengths_ref[d], doc, doc[:1, :])
        out_ref[d * SLOTS : (d + 1) * SLOTS, :] = doc.astype(jnp.bfloat16)
    lane = lax.broadcasted_iota(jnp.int32, (16, DIM), 1)
    facts = jnp.zeros((16, DIM), jnp.int32)
    for d in range(DOCS):
        facts = jnp.where(lane == d, lengths_ref[d], facts)
    out_ref[DOCS * SLOTS :, :] = facts.astype(jnp.float32).astype(jnp.bfloat16)


def pack(lengths, docs, queries):
    return pl.pallas_call(
        pack_kernel,
        out_shape=(pltpu.VMEM((PAY, DIM), jnp.bfloat16), pltpu.VMEM(queries.shape, jnp.bfloat16)),
        in_specs=[spec(pltpu.SMEM), spec(pltpu.VMEM), spec(pltpu.VMEM)],
        out_specs=(spec(pltpu.VMEM), spec(pltpu.VMEM)),
        cost_estimate=pl.CostEstimate(flops=10**6, bytes_accessed=10**6, transcendentals=0),
        name="pack",
    )(lengths, docs, queries)


def lower_half(shift, axis):
    return (lax.broadcasted_iota(jnp.int32, (8, 128), axis) // shift) % 2 == 0


def merge_max(a, b, shift):
    low = lower_half(shift, 0)
    return jnp.maximum(jnp.where(low, a, b), pltpu.roll(jnp.where(low, b, a), shift, 0))


def merge_sum(a, b, shift):
    return jnp.where(lower_half(shift, 1), a + pltpu.roll(a, 128 - shift, 1), b + pltpu.roll(b, shift, 1))


def doc_sources(me):
    flips = {"xb": 48, "yb": 68, "zb": 3}
    first, second, third = (
        jnp.where((me >> 3) & 1 == 0, flips[a], flips[b]) for a, b in zip(DOC_STEPS[0], DOC_STEPS[1])
    )
    masks = [0, first, second, first ^ second]
    return [me ^ m for m in masks] + [me ^ third ^ m for m in masks]


def block_member(me, block):
    yh, x1, x0, core, yl, z1, z0 = [(me >> k) & 1 for k in (6, 5, 4, 3, 2, 1, 0)]
    mine = (x0 ^ x1) | (yl ^ yh) << 1 | (z0 ^ z1) << 2
    flips = []
    for steps in QUERY_STEPS:
        flips.append(sum(((block >> k) & 1) << QUERY_STEPS[0].index(dim) for k, dim in enumerate(steps)))
    other = block >> 3
    return ((core ^ other) << 3) | (mine ^ jnp.where(core == other, flips[0], flips[1]))


def score_kernel(sizes, blocks, final, facts_ref, *refs):
    doc_refs, rest = refs[: len(sizes)], refs[len(sizes) :]
    query_refs, rest = rest[:2], rest[2:]
    if final:
        earlier_ref, rest = rest[0], rest[1:]
    out_ref, rows, best, owner, carry = rest[:5]
    doc_count = DOCS * sum(sizes)
    total = jnp.int32(0)
    first = 0
    for size, doc_ref in zip(sizes, doc_refs):
        for p in range(size):
            part = first + p
            for d in range(DOCS):
                source = p * PAY + d * SLOTS
                rows[pl.ds(pl.multiple_of(total * 16, 16), SLOTS), :] = doc_ref[source : source + SLOTS, :]
                for k in range(SLOTS // 16):
                    owner[total + k] = part * DOCS + d
                total = total + ((facts_ref[part * 8 + d] + 15) >> 4)
        first += size
    for k in range(STEPS[-1]):
        owner[total + k] = doc_count
    carry[...] = jnp.full_like(carry, neg_fill)

    def step(groups, base, last):
        ids = [owner[base + g] for g in range(groups)]
        drop = [jnp.where(a == b, 0.0, neg_fill) for a, b in zip(ids, [last] + ids[:-1])]
        block_rows = rows[pl.ds(pl.multiple_of(base * 16, 16), groups * 16), :]
        for b in range(blocks):
            similar = lax.dot_general(
                block_rows,
                query_refs[b // 8][b % 8 * 256 : (b % 8 + 1) * 256, :],
                (((1,), (1,)), ((), ())),
                preferred_element_type=jnp.float32,
            )
            for h in range(2):
                run = carry[2 * b + h]
                for g in range(groups):
                    tile = similar[16 * g : 16 * g + 16, 128 * h : 128 * h + 128]
                    run = jnp.maximum(jnp.maximum(tile[:8], tile[8:]), run + drop[g])
                    best[2 * b + h, pl.ds(pl.multiple_of(ids[g] * 8, 8), 8), :] = run
                carry[2 * b + h] = run
        return ids[-1]

    base, last = jnp.int32(0), jnp.int32(-1)
    for groups in STEPS:
        up = groups - 1 if groups == STEPS[-1] else 0
        count = (total - base + up) >> (groups.bit_length() - 1)
        last = lax.fori_loop(
            0, count, lambda i, last, groups=groups, base=base: step(groups, base + i * groups, last), last
        )
        base = base + count * groups

    for part in range(sum(sizes)):
        columns = []
        for half in range(2 * blocks):
            v = [best[half, (part * 8 + d) * 8 : (part * 8 + d + 1) * 8, :] for d in range(8)]
            for shift in (1, 2, 4):
                v = [merge_max(v[2 * k], v[2 * k + 1], shift) for k in range(len(v) // 2)]
            columns.append(v[0])
        for shift in (1, 2, 4, 8, 16):
            columns = [merge_sum(columns[2 * k], columns[2 * k + 1], shift) for k in range(len(columns) // 2)]
        if final:
            rest[5][doc_count + part * 8 : doc_count + part * 8 + 8, :] = columns[0]
        else:
            out_ref[part * 8 : part * 8 + 8, :] = columns[0]
    if final:
        scores, turned = rest[5:]
        me = lax.axis_index("d")
        scores[:doc_count, :] = earlier_ref[...]
        for part, source in enumerate(doc_sources(me)):
            ids = source * DOCS + lax.broadcasted_iota(jnp.int32, (8, 128), 0)
            scores[64 + part * 8 : 64 + part * 8 + 8, :] = ids.astype(jnp.float32)
        turned[...] = scores[...].T
        for b in range(blocks):
            quarters = [turned[pl.ds(2 * b + h, 4, stride=32), :] for h in range(2)]
            out_ref[block_member(me, b)] = jnp.concatenate(quarters)


def score(facts, docs, queries, earlier=None):
    sizes = [d.shape[0] // PAY for d in docs]
    doc_count = DOCS * sum(sizes)
    blocks = sum(q.shape[0] for q in queries) // 256
    final = earlier is not None
    operands = [*docs, *queries] + ([earlier] if final else [])
    return pl.pallas_call(
        functools.partial(score_kernel, sizes, blocks, final),
        out_shape=pltpu.VMEM((16, 8, 128) if final else (doc_count, 128), jnp.float32),
        in_specs=[spec(pltpu.SMEM)] + [spec(pltpu.VMEM)] * len(operands),
        out_specs=spec(pltpu.VMEM),
        scratch_shapes=[
            pltpu.VMEM((doc_count * SLOTS + STEPS[-1] * 16, DIM), jnp.bfloat16),
            pltpu.VMEM((blocks * 2, (doc_count + 1) * 8, 128), jnp.float32),
            pltpu.SMEM((doc_count * 8 + STEPS[-1],), jnp.int32),
            pltpu.VMEM((blocks * 2, 8, 128), jnp.float32),
        ]
        + ([pltpu.VMEM((128, 128), jnp.float32)] * 2 if final else []),
        compiler_params=pltpu.CompilerParams(vmem_limit_bytes=24 * 2**20),
        cost_estimate=pl.CostEstimate(flops=6 * 10**9, bytes_accessed=10**6, transcendentals=0),
        name="score",
    )(facts, *operands)


def lengths_of(docs):
    facts = [d[(k + 1) * PAY - 16, :DOCS] for d in docs for k in range(d.shape[0] // PAY)]
    return jnp.stack(facts).astype(jnp.int32).reshape(-1)


def finish_kernel(positives_ref, given_ref, out_ref):
    lane = lax.broadcasted_iota(jnp.int32, (8, 128), 1)
    row = lax.broadcasted_iota(jnp.int32, (8, 128), 0)
    wanted = jnp.zeros((8, 128), jnp.int32)
    for q in range(QUERIES):
        wanted = jnp.where(row == q, positives_ref[q], wanted)
    wanted = wanted.astype(jnp.float32)
    count = given_ref.shape[0]
    given = [given_ref[k] for k in range(count)]
    real = [jnp.where(lane < 64, g, neg_fill) for g in given]
    peak = jnp.max(functools.reduce(jnp.maximum, real), axis=1, keepdims=True)
    total = jnp.sum(sum(jnp.where(lane < 64, jnp.exp(r - peak), 0.0) for r in real), axis=1, keepdims=True)
    chosen = [jnp.where((lane < 64) & (pltpu.roll(g, 64, 1) == wanted), g, 0.0) for g in given]
    loss = peak + jnp.log(total) - jnp.sum(sum(chosen), axis=1, keepdims=True)
    out_ref[...] = jnp.sum(jnp.where(row == lane, loss, 0.0), axis=0)[:QUERIES]


def finish(positives, given):
    return pl.pallas_call(
        finish_kernel,
        out_shape=jax.ShapeDtypeStruct((QUERIES,), jnp.float32),
        in_specs=[spec(pltpu.SMEM), spec(pltpu.VMEM)],
        out_specs=spec(pltpu.VMEM),
        name="finish",
    )(positives, given)


def local(queries, documents, lengths, positives):
    query = queries.reshape(QUERIES * TOKENS, DIM)
    got = swap(query, QUERY_STEPS, 0)
    own, query = pack(lengths, documents, query)
    first = swap(own, DOC_STEPS, 0)
    second = swap(own, DOC_STEPS, 1)
    third = swap(own, DOC_STEPS, 2)
    query = jnp.concatenate([query, got])
    query = jnp.concatenate([query, swap(query, QUERY_STEPS, 1)])
    query = jnp.concatenate([query, swap(query, QUERY_STEPS, 2)])
    near = [own, first, second, swap(first, DOC_STEPS, 1)]
    far = [third, swap(jnp.concatenate(near[1:3]), DOC_STEPS, 2), swap(near[3], DOC_STEPS, 2)]
    queries = [query, swap_cores(query)]
    given = score(lengths_of(near), near, queries)
    given = score(lengths_of(far), far, queries, given)
    given = lax.all_to_all(given, "d", 0, 0, tiled=True, axis_index_groups=owner_groups())
    return finish(positives, given)


def solution(mesh):
    flat = Mesh(mesh.devices.reshape(-1), ("d",))
    placed = P("d")
    return jax.shard_map(local, mesh=flat, in_specs=(placed,) * 4, out_specs=placed, check_vma=False)
```

```python
import functools

import jax
import jax.numpy as jnp
from jax import lax
from jax.experimental import pallas as pl
from jax.experimental.pallas import tpu as pltpu
from jax.sharding import Mesh, PartitionSpec as P


neg_fill = -1e30
QUERIES, TOKENS, DOCS, SLOTS, DIM = 8, 32, 8, 128, 128
PAY = DOCS * SLOTS + 16
STEPS = (64, 16)


def index(x, y, z, core):
    return (((y // 2 * 4 + x) * 2 + core) * 2 + y % 2) * 4 + z


def everywhere():
    return [(x, y, z, c) for x in range(4) for y in range(4) for z in range(4) for c in range(2)]


def across(dim, place):
    axis = "xyz".index(dim[0])
    moved = list(place)
    moved[axis] = place[axis] ^ 1 if dim[1] == "a" else 3 - place[axis]
    return tuple(moved)


def side(dim, place):
    at = place["xyz".index(dim[0])]
    return ((0, 1, 1, 0) if dim[1] == "a" else (0, 0, 1, 1))[at]


DOC_STEPS = (("xb", "yb", "zb"), ("yb", "zb", "xb"))
QUERY_STEPS = (("xa", "ya", "za"), ("ya", "za", "xa"))


def swap(array, steps, at):
    pairs = [(index(*p), index(*across(steps[p[3]][at], p))) for p in everywhere()]
    return lax.ppermute(array, "d", pairs)


def swap_cores(array):
    pairs = [(index(x, y, z, c), index(x, y, z, 1 - c)) for x, y, z, c in everywhere()]
    return lax.ppermute(array, "d", pairs)


def member(place):
    return sum(side(dim, place) << k for k, dim in enumerate(QUERY_STEPS[place[3]]))


def member(place):
    return place[3] * 8 + sum(side(dim, place) << k for k, dim in enumerate(QUERY_STEPS[0]))


def owner_groups():
    groups = {}
    for p in everywhere():
        groups.setdefault(tuple(side(dim, p) for dim in DOC_STEPS[0]), []).append(p)
    return [[index(*p) for p in sorted(g, key=member)] for g in groups.values()]


def spec(space):
    return pl.BlockSpec(memory_space=space)


def pack_kernel(lengths_ref, docs_ref, queries_ref, out_ref, query_out):
    query_out[...] = queries_ref[...]
    row = lax.broadcasted_iota(jnp.int32, (SLOTS, DIM), 0)
    for d in range(DOCS):
        doc = docs_ref[d].astype(jnp.float32)
        doc = jnp.where(row < lengths_ref[d], doc, doc[:1, :])
        out_ref[d * SLOTS : (d + 1) * SLOTS, :] = doc.astype(jnp.bfloat16)
    lane = lax.broadcasted_iota(jnp.int32, (16, DIM), 1)
    facts = jnp.zeros((16, DIM), jnp.int32)
    for d in range(DOCS):
        facts = jnp.where(lane == d, lengths_ref[d], facts)
    out_ref[DOCS * SLOTS :, :] = facts.astype(jnp.float32).astype(jnp.bfloat16)


def pack(lengths, docs, queries):
    return pl.pallas_call(
        pack_kernel,
        out_shape=(pltpu.VMEM((PAY, DIM), jnp.bfloat16), pltpu.VMEM(queries.shape, jnp.bfloat16)),
        in_specs=[spec(pltpu.SMEM), spec(pltpu.VMEM), spec(pltpu.VMEM)],
        out_specs=(spec(pltpu.VMEM), spec(pltpu.VMEM)),
        cost_estimate=pl.CostEstimate(flops=10**6, bytes_accessed=10**6, transcendentals=0),
        name="pack",
    )(lengths, docs, queries)


def lower_half(shift, axis):
    return (lax.broadcasted_iota(jnp.int32, (8, 128), axis) // shift) % 2 == 0


def merge_max(a, b, shift):
    low = lower_half(shift, 0)
    return jnp.maximum(jnp.where(low, a, b), pltpu.roll(jnp.where(low, b, a), shift, 0))


def merge_sum(a, b, shift):
    return jnp.where(lower_half(shift, 1), a + pltpu.roll(a, 128 - shift, 1), b + pltpu.roll(b, shift, 1))


def doc_sources(me):
    flips = {"xb": 48, "yb": 68, "zb": 3}
    first, second, third = (
        jnp.where((me >> 3) & 1 == 0, flips[a], flips[b]) for a, b in zip(DOC_STEPS[0], DOC_STEPS[1])
    )
    masks = [0, first, second, first ^ second]
    return [me ^ m for m in masks] + [me ^ third ^ m for m in masks]


def block_member(me, block):
    yh, x1, x0, core, yl, z1, z0 = [(me >> k) & 1 for k in (6, 5, 4, 3, 2, 1, 0)]
    mine = (x0 ^ x1) | (yl ^ yh) << 1 | (z0 ^ z1) << 2
    flips = []
    for steps in QUERY_STEPS:
        flips.append(sum(((block >> k) & 1) << QUERY_STEPS[0].index(dim) for k, dim in enumerate(steps)))
    other = block >> 3
    return ((core ^ other) << 3) | (mine ^ jnp.where(core == other, flips[0], flips[1]))


def score_kernel(sizes, blocks, final, facts_ref, *refs):
    doc_refs, rest = refs[: len(sizes)], refs[len(sizes) :]
    query_refs, rest = rest[:2], rest[2:]
    if final:
        earlier_ref, rest = rest[0], rest[1:]
    out_ref, rows, best, owner, carry = rest[:5]
    doc_count = DOCS * sum(sizes)
    total = jnp.int32(0)
    first = 0
    for size, doc_ref in zip(sizes, doc_refs):
        for p in range(size):
            part = first + p
            for d in range(DOCS):
                source = p * PAY + d * SLOTS
                rows[pl.ds(pl.multiple_of(total * 16, 16), SLOTS), :] = doc_ref[source : source + SLOTS, :]
                for k in range(SLOTS // 16):
                    owner[total + k] = part * DOCS + d
                total = total + ((facts_ref[part * 8 + d] + 15) >> 4)
        first += size
    for k in range(STEPS[-1]):
        owner[total + k] = doc_count
    carry[...] = jnp.full_like(carry, neg_fill)

    def step(groups, base, last):
        ids = [owner[base + g] for g in range(groups)]
        drop = [jnp.where(a == b, 0.0, neg_fill) for a, b in zip(ids, [last] + ids[:-1])]
        block_rows = rows[pl.ds(pl.multiple_of(base * 16, 16), groups * 16), :]
        for b in range(blocks):
            similar = lax.dot_general(
                block_rows,
                query_refs[b // 8][b % 8 * 256 : (b % 8 + 1) * 256, :],
                (((1,), (1,)), ((), ())),
                preferred_element_type=jnp.float32,
            )
            for h in range(2):
                run = carry[2 * b + h]
                for g in range(groups):
                    tile = similar[16 * g : 16 * g + 16, 128 * h : 128 * h + 128]
                    run = jnp.maximum(jnp.maximum(tile[:8], tile[8:]), run + drop[g])
                    best[2 * b + h, pl.ds(pl.multiple_of(ids[g] * 8, 8), 8), :] = run
                carry[2 * b + h] = run
        return ids[-1]

    base, last = jnp.int32(0), jnp.int32(-1)
    for groups in STEPS:
        up = groups - 1 if groups == STEPS[-1] else 0
        count = (total - base + up) >> (groups.bit_length() - 1)
        last = lax.fori_loop(
            0, count, lambda i, last, groups=groups, base=base: step(groups, base + i * groups, last), last
        )
        base = base + count * groups

    for part in range(sum(sizes)):
        columns = []
        for half in range(2 * blocks):
            v = [best[half, (part * 8 + d) * 8 : (part * 8 + d + 1) * 8, :] for d in range(8)]
            for shift in (1, 2, 4):
                v = [merge_max(v[2 * k], v[2 * k + 1], shift) for k in range(len(v) // 2)]
            columns.append(v[0])
        for shift in (1, 2, 4, 8, 16):
            columns = [merge_sum(columns[2 * k], columns[2 * k + 1], shift) for k in range(len(columns) // 2)]
        if final:
            rest[5][doc_count + part * 8 : doc_count + part * 8 + 8, :] = columns[0]
        else:
            out_ref[part * 8 : part * 8 + 8, :] = columns[0]
    if final:
        scores, turned = rest[5:]
        me = lax.axis_index("d")
        scores[:doc_count, :] = earlier_ref[...]
        for part, source in enumerate(doc_sources(me)):
            ids = source * DOCS + lax.broadcasted_iota(jnp.int32, (8, 128), 0)
            scores[64 + part * 8 : 64 + part * 8 + 8, :] = ids.astype(jnp.float32)
        turned[...] = scores[...].T
        for b in range(blocks):
            quarters = [turned[pl.ds(2 * b + h, 4, stride=32), :] for h in range(2)]
            out_ref[block_member(me, b)] = jnp.concatenate(quarters)


def score(facts, docs, queries, earlier=None):
    sizes = [d.shape[0] // PAY for d in docs]
    doc_count = DOCS * sum(sizes)
    blocks = sum(q.shape[0] for q in queries) // 256
    final = earlier is not None
    operands = [*docs, *queries] + ([earlier] if final else [])
    return pl.pallas_call(
        functools.partial(score_kernel, sizes, blocks, final),
        out_shape=pltpu.VMEM((16, 8, 128) if final else (doc_count, 128), jnp.float32),
        in_specs=[spec(pltpu.SMEM)] + [spec(pltpu.VMEM)] * len(operands),
        out_specs=spec(pltpu.VMEM),
        scratch_shapes=[
            pltpu.VMEM((doc_count * SLOTS + STEPS[-1] * 16, DIM), jnp.bfloat16),
            pltpu.VMEM((blocks * 2, (doc_count + 1) * 8, 128), jnp.float32),
            pltpu.SMEM((doc_count * 8 + STEPS[-1],), jnp.int32),
            pltpu.VMEM((blocks * 2, 8, 128), jnp.float32),
        ]
        + ([pltpu.VMEM((128, 128), jnp.float32)] * 2 if final else []),
        compiler_params=pltpu.CompilerParams(vmem_limit_bytes=24 * 2**20),
        cost_estimate=pl.CostEstimate(flops=6 * 10**9, bytes_accessed=10**6, transcendentals=0),
        name="score",
    )(facts, *operands)


def lengths_of(docs):
    facts = [d[(k + 1) * PAY - 16, :DOCS] for d in docs for k in range(d.shape[0] // PAY)]
    return jnp.stack(facts).astype(jnp.int32).reshape(-1)


def finish_kernel(positives_ref, given_ref, out_ref):
    lane = lax.broadcasted_iota(jnp.int32, (8, 128), 1)
    row = lax.broadcasted_iota(jnp.int32, (8, 128), 0)
    wanted = jnp.zeros((8, 128), jnp.int32)
    for q in range(QUERIES):
        wanted = jnp.where(row == q, positives_ref[q], wanted)
    wanted = wanted.astype(jnp.float32)
    count = given_ref.shape[0]
    given = [given_ref[k] for k in range(count)]
    real = [jnp.where(lane < 64, g, neg_fill) for g in given]
    peak = jnp.max(functools.reduce(jnp.maximum, real), axis=1, keepdims=True)
    total = jnp.sum(sum(jnp.where(lane < 64, jnp.exp(r - peak), 0.0) for r in real), axis=1, keepdims=True)
    chosen = [jnp.where((lane < 64) & (pltpu.roll(g, 64, 1) == wanted), g, 0.0) for g in given]
    loss = peak + jnp.log(total) - jnp.sum(sum(chosen), axis=1, keepdims=True)
    out_ref[...] = jnp.sum(jnp.where(row == lane, loss, 0.0), axis=0)[:QUERIES]


def finish(positives, given):
    return pl.pallas_call(
        finish_kernel,
        out_shape=jax.ShapeDtypeStruct((QUERIES,), jnp.float32),
        in_specs=[spec(pltpu.SMEM), spec(pltpu.VMEM)],
        out_specs=spec(pltpu.VMEM),
        name="finish",
    )(positives, given)


def local(queries, documents, lengths, positives):
    query = queries.reshape(QUERIES * TOKENS, DIM)
    got = swap(query, QUERY_STEPS, 0)
    own, query = pack(lengths, documents, query)
    first = swap(own, DOC_STEPS, 0)
    second = swap(own, DOC_STEPS, 1)
    third = swap(own, DOC_STEPS, 2)
    query = jnp.concatenate([query, got])
    query = jnp.concatenate([query, swap(query, QUERY_STEPS, 1)])
    query = jnp.concatenate([query, swap(query, QUERY_STEPS, 2)])
    near = [own, first, second, swap(first, DOC_STEPS, 1)]
    two = lax.dynamic_update_slice(jnp.zeros((2 * PAY, DIM), jnp.bfloat16), first, (0, 0))
    two = lax.dynamic_update_slice(lax.optimization_barrier(two), second, (PAY, 0))
    far = [third, swap(two, DOC_STEPS, 2), swap(near[3], DOC_STEPS, 2)]
    queries = [query, swap_cores(query)]
    given = score(lengths_of(near), near, queries)
    given = score(lengths_of(far), far, queries, given)
    given = lax.all_to_all(given, "d", 0, 0, tiled=True, axis_index_groups=owner_groups())
    return finish(positives, given)


def solution(mesh):
    flat = Mesh(mesh.devices.reshape(-1), ("d",))
    placed = P("d")
    return jax.shard_map(local, mesh=flat, in_specs=(placed,) * 4, out_specs=placed, check_vma=False)
```
